16 devices in a mesh: dp: 2 (over y, z), tp: 8 (over x, core).
Axes of the slice: x: 4, y: 2, z: 1, core: 2. Of those that a mesh axis runs over, the one named last changes fastest.
The devices are a block of a 4x4x8 slice.
Arguments:
- act_in: bfloat16 [512, 5120], P('dp'), parts along dimension 0
- w_qkv: bfloat16 [2, 5120, 40, 3, 128], P(None, None, 'tp')
- w_out: bfloat16 [2, 40, 128, 5120], P(None, 'tp')
- w_up: bfloat16 [2, 5120, 20480], P(None, None, 'tp')
- w_down: bfloat16 [2, 20480, 5120], P(None, 'tp')
- gain_one: float32 [2, 5120], replicated
- gain_two: float32 [2, 5120], replicated
Outputs:
- output: bfloat16 [512, 5120], P('dp'), parts along dimension 0
There are 2 independent parts. The reference program is written for one: setup_inputs(seed, part) draws one part's arguments, and reference() takes and returns one part's arrays. A program takes and returns all parts, laid end to end along the dimension named above; an argument that names none is the same for every part.
All inputs are finite; a program needn't handle non-finite values.
Results may differ from the reference program's by a relative error of at most 0.0165387.
Values are sent between devices in bfloat16 or wider.
A program may use at most 768 MiB of HBM per device.

```python
import math
import jax
import jax.numpy as jnp
from jax import lax

SEQ_LEN = 256
MODEL_DIM = 5120
NUM_HEADS = 40
FFN_DIM = 20480
NUM_LAYERS = 2

HEAD_DIM = MODEL_DIM // NUM_HEADS
SCORE_SCALE = 1.0 / math.sqrt(HEAD_DIM)
ROW_BLOCK = math.gcd(SEQ_LEN, 2 ** int(math.log2(max(8, 2 ** 24 // (NUM_HEADS * SEQ_LEN)))))


def setup_inputs(seed: int = 0, part: int = 0) -> dict:
    part_key = jax.random.fold_in(jax.random.key(seed), part)
    key_common, key_noise = jax.random.split(part_key)
    shared_mean = jax.random.normal(key_common, (1, MODEL_DIM), jnp.float32)
    token_noise = jax.random.normal(key_noise, (SEQ_LEN, MODEL_DIM), jnp.float32)
    weight_keys = jax.random.split(jax.random.key(seed + 1), 6)
    w_qkv = jax.random.normal(weight_keys[0], (NUM_LAYERS, MODEL_DIM, NUM_HEADS, 3, HEAD_DIM), jnp.float32) * MODEL_DIM ** -0.5
    w_out = jax.random.normal(weight_keys[1], (NUM_LAYERS, NUM_HEADS, HEAD_DIM, MODEL_DIM), jnp.float32) * MODEL_DIM ** -0.5
    w_up = jax.random.normal(weight_keys[2], (NUM_LAYERS, MODEL_DIM, FFN_DIM), jnp.float32) * MODEL_DIM ** -0.5
    w_down = jax.random.normal(weight_keys[3], (NUM_LAYERS, FFN_DIM, MODEL_DIM), jnp.float32) * FFN_DIM ** -0.5
    gain_one = jax.random.uniform(weight_keys[4], (NUM_LAYERS, MODEL_DIM), jnp.float32, 0.5, 1.5)
    gain_two = jax.random.uniform(weight_keys[5], (NUM_LAYERS, MODEL_DIM), jnp.float32, 0.5, 1.5)
    return {
        "act_in": (shared_mean + token_noise).astype(jnp.bfloat16),
        "w_qkv": w_qkv.astype(jnp.bfloat16),
        "w_out": w_out.astype(jnp.bfloat16),
        "w_up": w_up.astype(jnp.bfloat16),
        "w_down": w_down.astype(jnp.bfloat16),
        "gain_one": gain_one,
        "gain_two": gain_two,
    }


def layer_norm(act_rows, gain_vec):
    rows_f32 = act_rows.astype(jnp.float32)
    centred = rows_f32 - jnp.mean(rows_f32, axis=-1, keepdims=True)
    var_rows = jnp.mean(centred * centred, axis=-1, keepdims=True)
    return (centred * lax.rsqrt(var_rows + 1e-5) * gain_vec).astype(jnp.bfloat16)


def causal_attention(query_rows, key_rows, value_rows):
    key_pos = jnp.arange(SEQ_LEN)
    key_f32 = key_rows.astype(jnp.float32)
    value_f32 = value_rows.astype(jnp.float32)

    def one_block(blk_idx):
        row_start = blk_idx * ROW_BLOCK
        q_blk = lax.dynamic_slice_in_dim(query_rows, row_start, ROW_BLOCK, axis=0).astype(jnp.float32)
        scores = jnp.einsum("qhd,khd->hqk", q_blk, key_f32) * SCORE_SCALE
        q_pos = row_start + jnp.arange(ROW_BLOCK)
        scores = jnp.where(key_pos[None, None, :] <= q_pos[None, :, None], scores, -1e30)
        exp_scores = jnp.exp(scores - jnp.max(scores, axis=-1, keepdims=True))
        prob_sum = jnp.sum(exp_scores, axis=-1)
        mix_out = jnp.einsum("hqk,khd->qhd", exp_scores.astype(jnp.bfloat16).astype(jnp.float32), value_f32)
        return (mix_out / prob_sum.T[:, :, None]).astype(jnp.bfloat16)

    blocks = lax.map(one_block, jnp.arange(SEQ_LEN // ROW_BLOCK))
    return blocks.reshape(SEQ_LEN, NUM_HEADS, HEAD_DIM)


def reference(act_in, w_qkv, w_out, w_up, w_down, gain_one, gain_two):
    def layer_step(act_rows, layer_weights):
        qkv_mat, out_mat, up_mat, down_mat, norm_one, norm_two = layer_weights
        normed = layer_norm(act_rows, norm_one)
        qkv_rows = jnp.dot(normed, qkv_mat.reshape(MODEL_DIM, 3 * MODEL_DIM), preferred_element_type=jnp.float32).astype(jnp.bfloat16)
        qkv_rows = qkv_rows.reshape(SEQ_LEN, NUM_HEADS, 3, HEAD_DIM)
        attn_rows = causal_attention(qkv_rows[:, :, 0], qkv_rows[:, :, 1], qkv_rows[:, :, 2])
        branch = jnp.dot(attn_rows.reshape(SEQ_LEN, MODEL_DIM), out_mat.reshape(MODEL_DIM, MODEL_DIM), preferred_element_type=jnp.float32)
        act_rows = (act_rows.astype(jnp.float32) + branch).astype(jnp.bfloat16)
        normed = layer_norm(act_rows, norm_two)
        hidden = jax.nn.gelu(jnp.dot(normed, up_mat, preferred_element_type=jnp.float32), approximate=True).astype(jnp.bfloat16)
        branch = jnp.dot(hidden, down_mat, preferred_element_type=jnp.float32)
        act_rows = (act_rows.astype(jnp.float32) + branch).astype(jnp.bfloat16)
        return act_rows, None

    final_rows = lax.scan(layer_step, act_in, (w_qkv, w_out, w_up, w_down, gain_one, gain_two))[0]
    return final_rows
```

```python
import functools
import math

import jax
import jax.numpy as jnp
from jax import lax
from jax.experimental import pallas as pl
from jax.experimental.pallas import tpu as pltpu
from jax.sharding import PartitionSpec as P

F32 = jnp.float32
BF16 = jnp.bfloat16
SLOTS = 12
LOADS = 24
PAIR, M1R, M1L, M2R, M2L, M3R, M3L = 0, 4, 5, 6, 7, 8, 9
STAT = 10
OWN_RA, OWN_RB, OWN_LA, OWN_LB, FWD_R, FWD_L = 18, 19, 20, 21, 22, 23
SH_OWN, SH_LA, SH_LB, SH_RA, SH_RB, SH_OA, SH_OB = 24, 25, 26, 27, 28, 29, 30
KINDS = 31


def layer_kernel(
    num_layers, num_chips, heads, head_dim,
    x_hbm, wq, wo, w1, w2, g1, g2, out,
    xg, a_buf, acc, pb, pr, sb, rb, qkv, o_buf, h_buf, st, mb, rsb, w,
    wsem, xsem, ssem, rsem,
):
    seq = xg.shape[1]
    bw = xg.shape[2]
    half = seq // 2
    hw = bw // 2
    model_dim = num_chips * bw
    tp = 2 * num_chips
    me = lax.axis_index("tp")
    chip = me // 2
    core = me % 2
    mine = pl.ds(pl.multiple_of(core * half, half), half)
    theirs = pl.ds(pl.multiple_of((1 - core) * half, half), half)

    def chip_at(r):
        return lax.rem(chip + r, num_chips)

    def block(r):
        return pl.ds(pl.multiple_of(chip_at(r) * bw, bw), bw)

    right = chip_at(1) * 2 + core
    left = chip_at(3) * 2 + core
    partner = chip * 2 + (1 - core)
    half_a = pl.ds(0, hw)
    half_b = pl.ds(hw, hw)

    def copies(l, k):
        s = k % SLOTS
        res = []

        def slab(t, r, col):
            res.append((wq.at[l, t, block(r), :], w.at[s, :, pl.ds(col, head_dim)]))

        if k in (0, 2, 3, 5):
            r = {0: 0, 2: 1, 3: 3, 5: 2}[k]
            for t in range(10):
                slab(t, r, t * head_dim)
        elif k in (1, 4):
            for n, r in enumerate({1: (0, 1), 4: (3, 2)}[k]):
                for t in range(5):
                    slab(10 + t, r, n * hw + t * head_dim)
        elif k < 8:
            for n, r in enumerate({6: (2, 1), 7: (3, 0)}[k]):
                res.append((wo.at[l, :, block(r)], w.at[s, pl.ds(n * hw, hw), :]))
        elif k < 16:
            r = (0, 1, 3, 2)[(k - 8) // 2]
            res.append((w1.at[l, block(r), pl.ds((k % 2) * bw, bw)], w.at[s]))
        else:
            r = (2, 1, 3, 0)[(k - 16) // 2]
            res.append((w2.at[l, pl.ds((k % 2) * bw, bw), block(r)], w.at[s]))
        return [pltpu.make_async_copy(a, b, wsem.at[s]) for a, b in res]

    def load(l, k):
        for c in copies(l, k):
            c.start()

    def load_after(l, k):
        n = k + SLOTS
        if n < LOADS:
            load(l, n)
        else:
            @pl.when(l + 1 < num_layers)
            def _():
                load(l + 1, n - LOADS)

    def wait_w(k):
        s = k % SLOTS
        pltpu.make_async_copy(w.at[s], w.at[s], wsem.at[s]).wait()

    def rc(kind, src, dst, dev):
        return pltpu.make_async_remote_copy(
            src_ref=src, dst_ref=dst, send_sem=ssem.at[kind], recv_sem=rsem.at[kind],
            device_id={"tp": dev}, device_id_type=pl.DeviceIdType.MESH,
        )

    def msg(kind):
        if kind < 4:
            return rc(kind, pb.at[kind, theirs, :], pr.at[kind], partner)
        if kind < STAT:
            n = kind - M1R
            return rc(kind, sb.at[n], rb.at[n], right if n % 2 == 0 else left)
        if kind < STAT + 8:
            d, o = (kind - STAT) // 2, (kind - STAT) % 2
            dev = chip_at(d) * 2 + (core if o == 0 else 1 - core)
            return rc(kind, st.at[0, core], st.at[(4 - d) % 4, core], dev)
        if kind == OWN_RA:
            return rc(kind, xg.at[0, mine, half_a], xg.at[3, mine, half_a], right)
        if kind == OWN_RB:
            return rc(kind, xg.at[0, mine, half_b], xg.at[3, mine, half_b], right)
        if kind == OWN_LA:
            return rc(kind, xg.at[0, mine, half_a], xg.at[1, mine, half_a], left)
        if kind == OWN_LB:
            return rc(kind, xg.at[0, mine, half_b], xg.at[1, mine, half_b], left)
        if kind == FWD_R:
            return rc(kind, xg.at[3, mine, half_a], xg.at[2, mine, half_a], right)
        if kind == FWD_L:
            return rc(kind, xg.at[1, mine, half_b], xg.at[2, mine, half_b], left)
        if kind == SH_OWN:
            return rc(kind, xg.at[0, mine, :], xg.at[0, mine, :], partner)
        r, hf = {SH_LA: (3, half_a), SH_LB: (3, half_b), SH_RA: (1, half_a), SH_RB: (1, half_b),
                 SH_OA: (2, half_a), SH_OB: (2, half_b)}[kind]
        return rc(kind, xg.at[r, mine, hf], xg.at[r, mine, hf], partner)

    def send(*kinds):
        for kind in kinds:
            msg(kind).start()

    def recv(*kinds):
        for kind in kinds:
            msg(kind).wait_recv()

    def block_stats(r, h):
        x = xg[r, pl.ds(pl.multiple_of(h * half, half), half), :].astype(F32)
        mean = jnp.sum(x, axis=1, keepdims=True) * (1.0 / bw)
        d = x - mean
        m2 = jnp.sum(d * d, axis=1, keepdims=True)
        lane = lax.broadcasted_iota(jnp.int32, (half, 128), 1)
        both = jnp.where(lane == 0, mean, m2)
        st[r, h] = both.T[0:8, :]

    def combine_stats():
        for h in range(2):
            means = [st[r, h, 0:1, :] for r in range(num_chips)]
            m2s = [st[r, h, 1:2, :] for r in range(num_chips)]
            mean = sum(means[1:], means[0]) * (1.0 / num_chips)
            dev = [(m - mean) * (m - mean) for m in means]
            m2 = sum(m2s[1:], m2s[0]) + bw * sum(dev[1:], dev[0])
            rstd = lax.rsqrt(m2 * (1.0 / model_dim) + 1e-5)
            rows = pl.ds(h * half, half)
            mb[rows, :] = jnp.broadcast_to(mean, (128, half)).T
            rsb[rows, :] = jnp.broadcast_to(rstd, (128, half)).T

    def normalise(l, r, gain):
        base = chip_at(r) * bw

        def tile(n, c):
            cols = pl.ds(pl.multiple_of(n * 128, 128), 128)
            g = gain[:, pl.ds(pl.multiple_of(base + n * 128, 128), 128)]
            row = lax.broadcasted_iota(jnp.int32, g.shape, 0)
            g = jnp.sum(jnp.where(row == l, g, 0.0), axis=0, keepdims=True)
            x = xg[r, :, cols].astype(F32)
            a_buf[:, cols] = ((x - mb[...]) * rsb[...] * g).astype(BF16)
            return c

        lax.fori_loop(0, bw // 128, tile, 0)

    def cons_qkv(l, pos):
        r = (0, 1, 3, 2)[pos]
        main, extra, ecol = ((0, 1, 0), (2, 1, hw), (3, 4, 0), (5, 4, hw))[pos]
        normalise(l, r, g1)
        wait_w(main)
        if pos in (0, 2):
            wait_w(extra)
        nh = hw // head_dim

        def tile(n, c):
            third = n // 2
            slot = main + third * (extra - main)
            col = pl.multiple_of((n - 2 * third) * hw + third * ecol, hw)
            part = jnp.dot(a_buf[...], w[slot, :, pl.ds(col, hw)], preferred_element_type=F32)
            cols = pl.ds(pl.multiple_of(n * hw, hw), hw)
            if pos > 0:
                part = acc[:, cols] + part
            if pos < 3:
                acc[:, cols] = part
            else:
                for t in range(nh):
                    qkv[n * nh + t] = part[:, t * head_dim:(t + 1) * head_dim].astype(BF16)
            return c

        lax.fori_loop(0, 3, tile, 0)
        load_after(l, main)
        if pos in (1, 3):
            load_after(l, extra)

    def cons_up(l, pos):
        r = (0, 1, 3, 2)[pos]
        k0 = 8 + 2 * pos
        normalise(l, r, g2)
        wait_w(k0)
        wait_w(k0 + 1)

        def tile(n, c):
            slot = k0 % SLOTS + n // 2
            col = pl.multiple_of((n % 2) * hw, hw)
            part = jnp.dot(a_buf[...], w[slot, :, pl.ds(col, hw)], preferred_element_type=F32)
            cols = pl.ds(pl.multiple_of(n * hw, hw), hw)
            if pos > 0:
                part = acc[:, cols] + part
            if pos < 3:
                acc[:, cols] = part
            else:
                h_buf[:, cols] = jax.nn.gelu(part, approximate=True).astype(BF16)
            return c

        lax.fori_loop(0, 4, tile, 0)
        load_after(l, k0)
        load_after(l, k0 + 1)

    def prod_out(l, d):
        k = 6 if d in (2, 1) else 7
        row = 0 if d in (2, 3) else hw
        if row == 0:
            wait_w(k)

        def tile(n, c):
            cols = pl.ds(pl.multiple_of(n * hw, hw), hw)
            pb[d, :, cols] = jnp.dot(
                o_buf[...], w[k % SLOTS, pl.ds(row, hw), cols], preferred_element_type=F32).astype(BF16)
            return c

        lax.fori_loop(0, 2, tile, 0)
        if row:
            load_after(l, k)

    def prod_down(l, d):
        k0 = {2: 16, 1: 18, 3: 20, 0: 22}[d]
        s0 = k0 % SLOTS
        wait_w(k0)
        wait_w(k0 + 1)

        def tile(n, c):
            cols = pl.ds(pl.multiple_of(n * hw, hw), hw)
            part = jnp.dot(h_buf[:, 0:bw], w[s0, :, cols], preferred_element_type=F32)
            part += jnp.dot(h_buf[:, bw:2 * bw], w[s0 + 1, :, cols], preferred_element_type=F32)
            pb[d, :, cols] = part.astype(BF16)
            return c

        lax.fori_loop(0, 2, tile, 0)
        load_after(l, k0)
        load_after(l, k0 + 1)

    def pair_sum(d, cols):
        return pb[d, mine, cols].astype(F32) + pr[d, :, cols].astype(F32)

    def reduce_scatter(prod):
        prod(2)
        send(PAIR + 2)
        prod(1)
        send(PAIR + 1)
        recv(PAIR + 2)
        sb[0] = pair_sum(2, half_a).astype(BF16)
        sb[1] = pair_sum(2, half_b).astype(BF16)
        send(M1R, M1L)
        prod(3)
        send(PAIR + 3)
        recv(PAIR + 1)
        sb[2] = pair_sum(1, half_b).astype(BF16)
        send(M2R)
        prod(0)
        send(PAIR + 0)
        recv(PAIR + 3)
        sb[3] = pair_sum(3, half_a).astype(BF16)
        send(M2L)
        recv(M1R)
        sb[4] = (pair_sum(1, half_a) + rb[0].astype(F32)).astype(BF16)
        send(M3R)
        recv(M1L)
        sb[5] = (pair_sum(3, half_b) + rb[1].astype(F32)).astype(BF16)
        send(M3L)
        recv(PAIR + 0, M2L, M3R)
        xg[0, mine, half_a] = (xg[0, mine, half_a].astype(F32) + (
            pair_sum(0, half_a) + rb[3].astype(F32) + rb[4].astype(F32))).astype(BF16)
        recv(M2R, M3L)
        xg[0, mine, half_b] = (xg[0, mine, half_b].astype(F32) + (
            pair_sum(0, half_b) + rb[2].astype(F32) + rb[5].astype(F32))).astype(BF16)

    def gather(cons):
        stats = [STAT + n for n in range(1, 8)]
        block_stats(0, core)
        send(*stats)
        send(OWN_RA, OWN_LB, OWN_RB, OWN_LA, SH_OWN)
        recv(*stats)
        combine_stats()
        recv(SH_OWN)
        cons(0)
        recv(OWN_RA)
        send(FWD_R, SH_LA)
        recv(OWN_LB)
        send(FWD_L, SH_RB)
        recv(OWN_RB)
        send(SH_LB)
        recv(OWN_LA)
        send(SH_RA)
        recv(SH_RA, SH_RB)
        cons(1)
        recv(SH_LA, SH_LB)
        cons(2)
        recv(FWD_R)
        send(SH_OA)
        recv(FWD_L)
        send(SH_OB)
        recv(SH_OA, SH_OB)
        cons(3)
        for kind in range(KINDS):
            if kind != STAT:
                msg(kind).wait_send()

    def attention():
        scale = 1.0 / math.sqrt(head_dim)
        q_pos = lax.broadcasted_iota(jnp.int32, (seq, seq), 0)
        k_pos = lax.broadcasted_iota(jnp.int32, (seq, seq), 1)
        keep = k_pos <= q_pos
        for h in range(heads):
            s = lax.dot_general(qkv[3 * h], qkv[3 * h + 1], (((1,), (1,)), ((), ())),
                                preferred_element_type=F32) * scale
            s = jnp.where(keep, s, -1e30)
            p = jnp.exp(s - jnp.max(s, axis=1, keepdims=True))
            total = jnp.sum(p, axis=1, keepdims=True)
            mix = jnp.dot(p.astype(BF16), qkv[3 * h + 2], preferred_element_type=F32)
            o_buf[:, h * head_dim:(h + 1) * head_dim] = (mix / total).astype(BF16)

    x_copies = [pltpu.make_async_copy(x_hbm.at[:, block(r)], xg.at[r], xsem.at[r]) for r in range(num_chips)]
    for c in x_copies:
        c.start()
    for k in range(SLOTS):
        load(0, k)

    barrier = pltpu.get_barrier_semaphore()
    for n in range(1, tp):
        pl.semaphore_signal(barrier, inc=1, device_id={"tp": lax.rem(me + n, tp)},
                            device_id_type=pl.DeviceIdType.MESH)
    for c in x_copies:
        c.wait()

    def first_stats(n, c):
        block_stats(n // 2, n % 2)
        return c

    lax.fori_loop(0, 2 * num_chips, first_stats, 0)
    combine_stats()
    for pos in range(4):
        cons_qkv(0, pos)
    pl.semaphore_wait(barrier, tp - 1)

    def layer(l, c):
        attention()
        reduce_scatter(functools.partial(prod_out, l))
        gather(functools.partial(cons_up, l))
        reduce_scatter(functools.partial(prod_down, l))

        def next_qkv(pos):
            @pl.when(l + 1 < num_layers)
            def _():
                cons_qkv(l + 1, pos)

        gather(next_qkv)
        return c

    lax.fori_loop(0, num_layers, layer, 0)
    outs = [pltpu.make_async_copy(xg.at[r], out.at[:, block(r)], xsem.at[r]) for r in range(num_chips)]
    for c in outs:
        c.start()
    for c in outs:
        c.wait()


def solution(mesh):
    tp = mesh.shape["tp"]
    num_chips = tp // 2

    def device_fn(act_in, w_qkv, w_out, w_up, w_down, gain_one, gain_two):
        seq, model_dim = act_in.shape
        num_layers, _, heads, _, head_dim = w_qkv.shape
        ffn = w_up.shape[2]
        bw = model_dim // num_chips
        half, hw = seq // 2, bw // 2
        wq = jnp.transpose(w_qkv, (0, 2, 3, 1, 4)).reshape(num_layers, heads * 3, model_dim, head_dim)
        wo = w_out.reshape(num_layers, heads * head_dim, model_dim)
        vmem = pl.BlockSpec(memory_space=pltpu.VMEM)
        hbm = pl.BlockSpec(memory_space=pl.ANY)
        return pl.pallas_call(
            functools.partial(layer_kernel, num_layers, num_chips, heads, head_dim),
            out_shape=jax.ShapeDtypeStruct((seq, model_dim), BF16),
            in_specs=[hbm] * 5 + [vmem] * 2,
            out_specs=hbm,
            scratch_shapes=[
                pltpu.VMEM((num_chips, seq, bw), BF16),
                pltpu.VMEM((seq, bw), BF16),
                pltpu.VMEM((seq, ffn), F32),
                pltpu.VMEM((num_chips, seq, bw), BF16),
                pltpu.VMEM((num_chips, half, bw), BF16),
                pltpu.VMEM((6, half, hw), BF16),
                pltpu.VMEM((6, half, hw), BF16),
                pltpu.VMEM((heads * 3, seq, head_dim), BF16),
                pltpu.VMEM((seq, heads * head_dim), BF16),
                pltpu.VMEM((seq, ffn), BF16),
                pltpu.VMEM((num_chips, 2, 8, 128), F32),
                pltpu.VMEM((seq, 128), F32),
                pltpu.VMEM((seq, 128), F32),
                pltpu.VMEM((SLOTS, bw, bw), BF16),
                pltpu.SemaphoreType.DMA((SLOTS,)),
                pltpu.SemaphoreType.DMA((num_chips,)),
                pltpu.SemaphoreType.DMA((KINDS,)),
                pltpu.SemaphoreType.DMA((KINDS,)),
            ],
            compiler_params=pltpu.CompilerParams(
                collective_id=0, has_side_effects=True, vmem_limit_bytes=60 * 2 ** 20),
            name="layers",
        )(act_in, wq, wo, w_up, w_down, gain_one, gain_two)

    return jax.shard_map(
        device_fn,
        mesh=mesh,
        in_specs=(
            P("dp", None),
            P(None, None, "tp", None, None),
            P(None, "tp", None, None),
            P(None, None, "tp"),
            P(None, "tp", None),
            P(None, None),
            P(None, None),
        ),
        out_specs=P("dp", None),
        check_vma=False,
    )
```

```python
import functools
import math

import jax
import jax.numpy as jnp
from jax import lax
from jax.experimental import pallas as pl
from jax.experimental.pallas import tpu as pltpu
from jax.sharding import PartitionSpec as P

F32 = jnp.float32
BF16 = jnp.bfloat16
SLOTS = 12
PAIR, M1R, M1L, M2R, M2L, M3R, M3L = 0, 4, 5, 6, 7, 8, 9
OWN_RA, OWN_RB, OWN_LA, OWN_LB, FWD_R, FWD_L = 10, 11, 12, 13, 14, 15
SH_OWN, SH_LA, SH_LB, SH_RA, SH_RB, SH_OA, SH_OB = 16, 17, 18, 19, 20, 21, 22
KINDS = 23
ORDER = (2, 1, 3, 0)


def layer_kernel(
    num_layers, num_chips, heads, head_dim,
    x_hbm, wq, wo, w1, w2, g1, g2, out,
    xg, a_buf, pb, pr, sb, rb, qkv, o_buf, h_buf, w,
    wsem, xsem, ssem, rsem,
):
    rows = xg.shape[2]
    bw = xg.shape[3]
    own = rows // 2
    hw = bw // 2
    model_dim = num_chips * bw
    tp = 2 * num_chips
    me = lax.axis_index("tp")
    chip = me // 2
    core = me % 2
    mine = pl.ds(pl.multiple_of(core * own, own), own)
    theirs = pl.ds(pl.multiple_of((1 - core) * own, own), own)
    scope = jax.named_scope

    def chip_at(r):
        return lax.rem(chip + r, num_chips)

    def block(r):
        return pl.ds(pl.multiple_of(chip_at(r) * bw, bw), bw)

    right = chip_at(1) * 2 + core
    left = chip_at(3) * 2 + core
    partner = chip * 2 + (1 - core)
    half_a = pl.ds(0, hw)
    half_b = pl.ds(hw, hw)

    def load(l, what, n, s):
        res = []

        def slab(t, r, col):
            res.append((wq.at[l, t, block(r), :], w.at[s, :, pl.ds(col, head_dim)]))

        if what == "q" and n < 4:
            for t in range(10):
                slab(t, n, t * head_dim)
        elif what == "q":
            for i in range(2):
                for t in range(5):
                    slab(10 + t, 2 * (n - 4) + i, i * hw + t * head_dim)
        elif what == "o":
            for i in range(2):
                res.append((wo.at[l, :, block(ORDER[2 * n + i])], w.at[s, pl.ds(i * hw, hw), :]))
        elif what == "u":
            res.append((w1.at[l, block(n % 4), pl.ds((n // 4) * bw, bw)], w.at[s]))
        else:
            res.append((w2.at[l, pl.ds((n % 2) * bw, bw), block(ORDER[n // 2])], w.at[s]))
        for a, b in res:
            pltpu.make_async_copy(a, b, wsem.at[s]).start()

    def load_next(l, what, n, s):
        @pl.when(l + 1 < num_layers)
        def _():
            load(l + 1, what, n, s)

    def wait_w(*slots):
        with scope("wwait"):
            for s in slots:
                pltpu.make_async_copy(w.at[s], w.at[s], wsem.at[s]).wait()

    def msg(h, kind):
        def rc(src, dst, dev):
            return pltpu.make_async_remote_copy(
                src_ref=src, dst_ref=dst, send_sem=ssem.at[h, kind], recv_sem=rsem.at[h, kind],
                device_id={"tp": dev}, device_id_type=pl.DeviceIdType.MESH,
            )

        def move(r_from, r_to, cols, dev):
            return rc(xg.at[h, r_from, mine, cols], xg.at[h, r_to, mine, cols], dev)

        if kind < 4:
            return rc(pb.at[h, kind, theirs, :], pr.at[h, kind], partner)
        if kind <= M3L:
            n = kind - M1R
            return rc(sb.at[h, n], rb.at[h, n], right if n % 2 == 0 else left)
        return move(*{
            OWN_RA: (0, 3, half_a, right), OWN_RB: (0, 3, half_b, right),
            OWN_LA: (0, 1, half_a, left), OWN_LB: (0, 1, half_b, left),
            FWD_R: (3, 2, half_a, right), FWD_L: (1, 2, half_b, left),
            SH_OWN: (0, 0, pl.ds(0, bw), partner),
            SH_LA: (3, 3, half_a, partner), SH_LB: (3, 3, half_b, partner),
            SH_RA: (1, 1, half_a, partner), SH_RB: (1, 1, half_b, partner),
            SH_OA: (2, 2, half_a, partner), SH_OB: (2, 2, half_b, partner),
        }[kind])

    def send(h, *kinds):
        for kind in kinds:
            msg(h, kind).start()

    def recv(h, *kinds):
        for kind in kinds:
            with scope("recv%d" % kind):
                msg(h, kind).wait_recv()

    def pair_sum(h, d, cols):
        return pb[h, d, mine, cols].astype(F32) + pr[h, d, :, cols].astype(F32)

    def ev1(h):
        recv(h, PAIR + 2)
        sb[h, 0] = pair_sum(h, 2, half_a).astype(BF16)
        sb[h, 1] = pair_sum(h, 2, half_b).astype(BF16)
        send(h, M1R, M1L)

    def ev2(h):
        recv(h, PAIR + 1)
        sb[h, 2] = pair_sum(h, 1, half_b).astype(BF16)
        recv(h, PAIR + 3)
        sb[h, 3] = pair_sum(h, 3, half_a).astype(BF16)
        send(h, M2R, M2L)

    def ev3(h):
        recv(h, M1R)
        sb[h, 4] = (pair_sum(h, 1, half_a) + rb[h, 0].astype(F32)).astype(BF16)
        send(h, M3R)
        recv(h, M1L)
        sb[h, 5] = (pair_sum(h, 3, half_b) + rb[h, 1].astype(F32)).astype(BF16)
        send(h, M3L)

    def ev4(h):
        recv(h, PAIR + 0, M2L, M3R)
        xg[h, 0, mine, half_a] = (xg[h, 0, mine, half_a].astype(F32) + (
            pair_sum(h, 0, half_a) + rb[h, 3].astype(F32) + rb[h, 4].astype(F32))).astype(BF16)
        send(h, OWN_RA, OWN_LA)
        recv(h, M2R, M3L)
        xg[h, 0, mine, half_b] = (xg[h, 0, mine, half_b].astype(F32) + (
            pair_sum(h, 0, half_b) + rb[h, 2].astype(F32) + rb[h, 5].astype(F32))).astype(BF16)
        send(h, OWN_LB, OWN_RB, SH_OWN)

    def ev5(h):
        recv(h, OWN_RA)
        send(h, FWD_R, SH_LA)
        recv(h, OWN_LB)
        send(h, FWD_L, SH_RB)

    def ev6(h):
        recv(h, OWN_LA)
        send(h, SH_RA)
        recv(h, OWN_RB)
        send(h, SH_LB)

    def ev7(h):
        recv(h, FWD_R)
        send(h, SH_OA)
        recv(h, FWD_L)
        send(h, SH_OB)

    def ev8(h):
        recv(h, SH_OWN, SH_LA, SH_LB, SH_RA, SH_RB, SH_OA, SH_OB)
        with scope("sent"):
            for kind in range(KINDS):
                msg(h, kind).wait_send()

    def normalise(l, h, gain):
        step_rows = 32

        def tile(n, c):
            rs = pl.ds(pl.multiple_of(n * step_rows, step_rows), step_rows)

            def x_of(r):
                return xg[h, r, rs, :].astype(F32)

            total = sum(jnp.sum(x_of(r), axis=1, keepdims=True) for r in range(num_chips))
            mean = total * (1.0 / model_dim)
            sq = 0.0
            for r in range(num_chips):
                d = x_of(r) - mean
                sq = sq + jnp.sum(d * d, axis=1, keepdims=True)
            rstd = lax.rsqrt(sq * (1.0 / model_dim) + 1e-5)
            for r in range(num_chips):
                g = gain[:, block(r)]
                pick = lax.broadcasted_iota(jnp.int32, g.shape, 0) == l
                g = jnp.sum(jnp.where(pick, g, 0.0), axis=0, keepdims=True)
                a_buf[r, rs, :] = ((x_of(r) - mean) * rstd * g).astype(BF16)
            return c

        with scope("norm"):
            lax.fori_loop(0, rows // step_rows, tile, 0)

    def dot_all(lhs, rhs):
        return sum(jnp.dot(a, b, preferred_element_type=F32) for a, b in zip(lhs, rhs))

    def attn_steps(l, h):
        my_rows = pl.ds(pl.multiple_of(h * rows, rows), rows)

        def ln():
            normalise(l, h, g1)

        def qkv_main():
            @pl.when(h == 0)
            def _():
                wait_w(0, 1, 2, 3)

            with scope("mm_qkv"):
                part = dot_all([a_buf[r] for r in range(4)], [w[r] for r in range(4)])
                for t in range(10):
                    qkv[t, my_rows, :] = part[:, t * head_dim:(t + 1) * head_dim].astype(BF16)

            @pl.when(h == 1)
            def _():
                for r in range(4):
                    load(l, "u", 4 + r, r)

        def qkv_rest():
            @pl.when(h == 0)
            def _():
                wait_w(4, 5)

            with scope("mm_qkv2"):
                part = dot_all([a_buf[r] for r in range(4)],
                               [w[4 + r // 2, :, pl.ds((r % 2) * hw, hw)] for r in range(4)])
                for t in range(5):
                    qkv[10 + t, my_rows, :] = part[:, t * head_dim:(t + 1) * head_dim].astype(BF16)

            @pl.when(h == 1)
            def _():
                load(l, "d", 0, 4)
                load(l, "d", 1, 5)

        def attend(static_h):
            keys = pl.ds(0, (static_h + 1) * rows)
            at = pl.ds(static_h * rows, rows)
            shape = (rows, (static_h + 1) * rows)
            q_pos = static_h * rows + lax.broadcasted_iota(jnp.int32, shape, 0)
            keep = lax.broadcasted_iota(jnp.int32, shape, 1) <= q_pos
            scale = 1.0 / math.sqrt(head_dim)

            @pl.when(h == static_h)
            def _():
                with scope("attn"):
                    for n in range(heads):
                        s = lax.dot_general(qkv[3 * n, at, :], qkv[3 * n + 1, keys, :], (((1,), (1,)), ((), ())),
                                            preferred_element_type=F32) * scale
                        s = jnp.where(keep, s, -1e30)
                        p = jnp.exp(s - jnp.max(s, axis=1, keepdims=True))
                        total = jnp.sum(p, axis=1, keepdims=True)
                        mix = jnp.dot(p.astype(BF16), qkv[3 * n + 2, keys, :], preferred_element_type=F32)
                        o_buf[:, n * head_dim:(n + 1) * head_dim] = (mix / total).astype(BF16)

        def attend_both():
            attend(0)
            attend(1)

        def prod(n):
            d = ORDER[n]
            s = 6 + n // 2
            if n % 2 == 0:
                @pl.when(h == 0)
                def _():
                    wait_w(s)

            with scope("mm_out"):
                pb[h, d] = jnp.dot(o_buf[...], w[s, pl.ds((n % 2) * hw, hw), :],
                                   preferred_element_type=F32).astype(BF16)
            send(h, PAIR + d)
            if n % 2 == 1:
                @pl.when(h == 1)
                def _():
                    load(l, "d", 2 + n // 2, s)

        return [ln, qkv_main, qkv_rest, attend_both] + [functools.partial(prod, n) for n in range(4)]

    def mlp_steps(l, h):
        def ln():
            normalise(l, h, g2)

        def up(n):
            base = 8 if n == 0 else 4 * h
            if n == 0:
                @pl.when(h == 0)
                def _():
                    wait_w(8, 9, 10, 11)
            else:
                wait_w(*[base + r for r in range(4)])
            with scope("mm_up"):
                part = dot_all([a_buf[r] for r in range(4)], [w[base + r] for r in range(4)])
                h_buf[:, pl.ds(n * bw, bw)] = jax.nn.gelu(part, approximate=True).astype(BF16)

            @pl.when(h == 1 - n)
            def _():
                for r in range(4):
                    load(l, "d", 4 + r, base + r)

            if n == 1:
                @pl.when(h == 1)
                def _():
                    load_next(l, "q", 4, 4)
                    load_next(l, "q", 5, 5)
                    load_next(l, "o", 0, 6)
                    load_next(l, "o", 1, 7)

        def prod(n):
            d = ORDER[n]
            s0, s1 = ((4, 0), (6, 2), (0, 8), (2, 10))[n]
            s = s0 + h * (s1 - s0)
            wait_w(s, s + 1)
            with scope("mm_down"):
                part = dot_all([h_buf[:, 0:bw], h_buf[:, bw:2 * bw]], [w[s], w[s + 1]])
                pb[h, d] = part.astype(BF16)
            send(h, PAIR + d)

            @pl.when(h == 0)
            def _():
                for i in range(2):
                    if n < 2:
                        load(l, "u", 4 + 2 * n + i, s0 + i)
                    else:
                        load(l, "d", 2 * (n - 2) + i, s0 + i)

            @pl.when(h == 1)
            def _():
                for i in range(2):
                    if n < 2:
                        load_next(l, "q", 2 * n + i, s1 + i)
                    else:
                        load_next(l, "u", 2 * (n - 2) + i, s1 + i)

        return [ln, functools.partial(up, 0), functools.partial(up, 1)] + [
            functools.partial(prod, n) for n in range(4)]

    def run(steps, h, after3, after4, guard):
        g = 1 - h

        def other(*events):
            if guard is None:
                for ev in events:
                    ev(g)
            else:
                @pl.when(guard)
                def _():
                    for ev in events:
                        ev(g)

        for n, step in enumerate(steps):
            step()
            if n == after3:
                other(ev3)
            if n == after4:
                other(ev4)
        ev1(h)
        ev2(h)
        other(ev5, ev6, ev7, ev8)

    def x_copy(h, r):
        return pltpu.make_async_copy(x_hbm.at[pl.ds(h * rows, rows), block(r)], xg.at[h, r], xsem.at[h, r])

    def out_copy(h, r):
        return pltpu.make_async_copy(xg.at[h, r], out.at[pl.ds(h * rows, rows), block(r)], xsem.at[h, r])

    for r in range(num_chips):
        x_copy(0, r).start()
    for r in range(4):
        load(0, "q", r, r)
    barrier = pltpu.get_barrier_semaphore()
    for n in range(1, tp):
        pl.semaphore_signal(barrier, inc=1, device_id={"tp": lax.rem(me + n, tp)},
                            device_id_type=pl.DeviceIdType.MESH)
    with scope("xwait"):
        for r in range(num_chips):
            x_copy(0, r).wait()
    for r in range(num_chips):
        x_copy(1, r).start()
    load(0, "q", 4, 4)
    load(0, "q", 5, 5)
    load(0, "o", 0, 6)
    load(0, "o", 1, 7)
    for r in range(4):
        load(0, "u", r, 8 + r)
    with scope("bar"):
        pl.semaphore_wait(barrier, tp - 1)
    for r in range(num_chips):
        x_copy(1, r).wait()

    def layer(l, c):
        def attn_half(h, c):
            run(attn_steps(l, h), h, 1, 7, l + h > 0)
            return c

        def mlp_half(h, c):
            run(mlp_steps(l, h), h, 1, 3, None)
            return c

        lax.fori_loop(0, 2, attn_half, 0)
        lax.fori_loop(0, 2, mlp_half, 0)
        return c

    lax.fori_loop(0, num_layers, layer, 0)
    ev3(1)
    ev4(1)
    for r in range(num_chips):
        out_copy(0, r).start()
    for ev in (ev5, ev6, ev7, ev8):
        ev(1)
    for r in range(num_chips):
        out_copy(1, r).start()
    with scope("outw"):
        for h in range(2):
            for r in range(num_chips):
                out_copy(h, r).wait()


def solution(mesh):
    tp = mesh.shape["tp"]
    num_chips = tp // 2

    def device_fn(act_in, w_qkv, w_out, w_up, w_down, gain_one, gain_two):
        seq, model_dim = act_in.shape
        num_layers, _, heads, _, head_dim = w_qkv.shape
        ffn = w_up.shape[2]
        bw = model_dim // num_chips
        half, hw = seq // 2, bw // 2
        wq = jnp.transpose(w_qkv, (0, 2, 3, 1, 4)).reshape(num_layers, heads * 3, model_dim, head_dim)
        wo = w_out.reshape(num_layers, heads * head_dim, model_dim)
        vmem = pl.BlockSpec(memory_space=pltpu.VMEM)
        hbm = pl.BlockSpec(memory_space=pl.ANY)
        return pl.pallas_call(
            functools.partial(layer_kernel, num_layers, num_chips, heads, head_dim),
            out_shape=jax.ShapeDtypeStruct((seq, model_dim), BF16),
            in_specs=[hbm] * 5 + [vmem] * 2,
            out_specs=hbm,
            scratch_shapes=[
                pltpu.VMEM((2, num_chips, half, bw), BF16),
                pltpu.VMEM((num_chips, half, bw), BF16),
                pltpu.VMEM((2, num_chips, half, bw), BF16),
                pltpu.VMEM((2, num_chips, half // 2, bw), BF16),
                pltpu.VMEM((2, 6, half // 2, hw), BF16),
                pltpu.VMEM((2, 6, half // 2, hw), BF16),
                pltpu.VMEM((heads * 3, seq, head_dim), BF16),
                pltpu.VMEM((half, heads * head_dim), BF16),
                pltpu.VMEM((half, ffn), BF16),
                pltpu.VMEM((SLOTS, bw, bw), BF16),
                pltpu.SemaphoreType.DMA((SLOTS,)),
                pltpu.SemaphoreType.DMA((2, num_chips)),
                pltpu.SemaphoreType.DMA((2, KINDS)),
                pltpu.SemaphoreType.DMA((2, KINDS)),
            ],
            compiler_params=pltpu.CompilerParams(
                collective_id=0, has_side_effects=True, vmem_limit_bytes=60 * 2 ** 20),
            name="layers",
        )(act_in, wq, wo, w_up, w_down, gain_one, gain_two)

    return jax.shard_map(
        device_fn,
        mesh=mesh,
        in_specs=(
            P("dp", None),
            P(None, None, "tp", None, None),
            P(None, "tp", None, None),
            P(None, None, "tp"),
            P(None, "tp", None),
            P(None, None),
            P(None, None),
        ),
        out_specs=P("dp", None),
        check_vma=False,
    )
```

```python
import functools
import math

import jax
import jax.numpy as jnp
from jax import lax
from jax.experimental import pallas as pl
from jax.experimental.pallas import tpu as pltpu
from jax.sharding import PartitionSpec as P

F32 = jnp.float32
BF16 = jnp.bfloat16
SLOTS = 12
PAIR, M1R, M1L, M2R, M2L, M3R, M3L = 0, 4, 5, 6, 7, 8, 9
OWN_RA, OWN_RB, OWN_LA, OWN_LB, FWD_R, FWD_L = 10, 11, 12, 13, 14, 15
SH_OWN, SH_LA, SH_LB, SH_RA, SH_RB, SH_OA, SH_OB = 16, 17, 18, 19, 20, 21, 22
KINDS = 23
ORDER = (2, 1, 3, 0)
SELF, OTHER = 0, 1


def layer_kernel(
    num_layers, num_chips, heads, head_dim,
    x_hbm, wq, wo, w1, w2, g1, g2, out,
    xg, a_buf, pb, pr, sb, rb, qkv, o_buf, h_buf, w,
    wsem, xsem, ssem, rsem,
):
    rows = xg.shape[2]
    bw = xg.shape[3]
    own = rows // 2
    hw = bw // 2
    model_dim = num_chips * bw
    tp = 2 * num_chips
    me = lax.axis_index("tp")
    chip = me // 2
    core = me % 2
    mine = pl.ds(pl.multiple_of(core * own, own), own)
    theirs = pl.ds(pl.multiple_of((1 - core) * own, own), own)
    scope = jax.named_scope

    def chip_at(r):
        return lax.rem(chip + r, num_chips)

    def block(r):
        return pl.ds(pl.multiple_of(chip_at(r) * bw, bw), bw)

    right = chip_at(1) * 2 + core
    left = chip_at(3) * 2 + core
    partner = chip * 2 + (1 - core)
    half_a = pl.ds(0, hw)
    half_b = pl.ds(hw, hw)

    def load(l, what, n, s):
        res = []

        def slab(t, r, col):
            res.append((wq.at[l, t, block(r), :], w.at[s, :, pl.ds(col, head_dim)]))

        if what == "q" and n < 4:
            for t in range(10):
                slab(t, n, t * head_dim)
        elif what == "q":
            for i in range(2):
                for t in range(5):
                    slab(10 + t, 2 * (n - 4) + i, i * hw + t * head_dim)
        elif what == "o":
            for i in range(2):
                res.append((wo.at[l, :, block(ORDER[2 * n + i])], w.at[s, pl.ds(i * hw, hw), :]))
        elif what == "u":
            res.append((w1.at[l, block(n % 4), pl.ds((n // 4) * bw, bw)], w.at[s]))
        else:
            res.append((w2.at[l, pl.ds((n % 2) * bw, bw), block(ORDER[n // 2])], w.at[s]))
        for a, b in res:
            pltpu.make_async_copy(a, b, wsem.at[s]).start()

    def load_next(l, what, n, s):
        @pl.when(l + 1 < num_layers)
        def _():
            load(l + 1, what, n, s)

    def wait_w(*slots):
        with scope("wwait"):
            for s in slots:
                pltpu.make_async_copy(w.at[s], w.at[s], wsem.at[s]).wait()

    def msg(h, kind):
        def rc(src, dst, dev):
            return pltpu.make_async_remote_copy(
                src_ref=src, dst_ref=dst, send_sem=ssem.at[h, kind], recv_sem=rsem.at[h, kind],
                device_id={"tp": dev}, device_id_type=pl.DeviceIdType.MESH,
            )

        def move(r_from, r_to, cols, dev):
            return rc(xg.at[h, r_from, mine, cols], xg.at[h, r_to, mine, cols], dev)

        if kind < 4:
            return rc(pb.at[h, kind, theirs, :], pr.at[h, kind], partner)
        if kind <= M3L:
            n = kind - M1R
            return rc(sb.at[h, n], rb.at[h, n], right if n % 2 == 0 else left)
        return move(*{
            OWN_RA: (0, 3, half_a, right), OWN_RB: (0, 3, half_b, right),
            OWN_LA: (0, 1, half_a, left), OWN_LB: (0, 1, half_b, left),
            FWD_R: (3, 2, half_a, right), FWD_L: (1, 2, half_b, left),
            SH_OWN: (0, 0, pl.ds(0, bw), partner),
            SH_LA: (3, 3, half_a, partner), SH_LB: (3, 3, half_b, partner),
            SH_RA: (1, 1, half_a, partner), SH_RB: (1, 1, half_b, partner),
            SH_OA: (2, 2, half_a, partner), SH_OB: (2, 2, half_b, partner),
        }[kind])

    def send(h, *kinds):
        for kind in kinds:
            msg(h, kind).start()

    def recv(h, *kinds):
        for kind in kinds:
            with scope("recv%d" % kind):
                msg(h, kind).wait_recv()

    def pair_sum(h, d, cols):
        return pb[h, d, mine, cols].astype(F32) + pr[h, d, :, cols].astype(F32)

    def ev1(h):
        recv(h, PAIR + 2)
        sb[h, 0] = pair_sum(h, 2, half_a).astype(BF16)
        sb[h, 1] = pair_sum(h, 2, half_b).astype(BF16)
        send(h, M1R, M1L)

    def ev2(h):
        recv(h, PAIR + 1)
        sb[h, 2] = pair_sum(h, 1, half_b).astype(BF16)
        recv(h, PAIR + 3)
        sb[h, 3] = pair_sum(h, 3, half_a).astype(BF16)
        send(h, M2R, M2L)

    def ev3(h):
        recv(h, M1R)
        sb[h, 4] = (pair_sum(h, 1, half_a) + rb[h, 0].astype(F32)).astype(BF16)
        send(h, M3R)
        recv(h, M1L)
        sb[h, 5] = (pair_sum(h, 3, half_b) + rb[h, 1].astype(F32)).astype(BF16)
        send(h, M3L)

    def ev4(h):
        recv(h, PAIR + 0, M2L, M3R)
        xg[h, 0, mine, half_a] = (xg[h, 0, mine, half_a].astype(F32) + (
            pair_sum(h, 0, half_a) + rb[h, 3].astype(F32) + rb[h, 4].astype(F32))).astype(BF16)
        send(h, OWN_RA)
        recv(h, M2R, M3L)
        xg[h, 0, mine, half_b] = (xg[h, 0, mine, half_b].astype(F32) + (
            pair_sum(h, 0, half_b) + rb[h, 2].astype(F32) + rb[h, 5].astype(F32))).astype(BF16)
        send(h, OWN_LB, OWN_LA, OWN_RB, SH_OWN)

    def ev5(h):
        recv(h, OWN_RA)
        send(h, FWD_R, SH_LA)
        recv(h, OWN_LB)
        send(h, FWD_L, SH_RB)

    def ev6(h):
        recv(h, OWN_LA)
        send(h, SH_RA)
        recv(h, OWN_RB)
        send(h, SH_LB)

    def ev7(h):
        recv(h, FWD_R)
        send(h, SH_OA)
        recv(h, FWD_L)
        send(h, SH_OB)

    def ev8(h):
        recv(h, SH_OWN, SH_LA, SH_LB, SH_RA, SH_RB, SH_OA, SH_OB)
        with scope("sent"):
            for kind in range(KINDS):
                msg(h, kind).wait_send()

    def normalise(l, h, gain):
        tiles = bw // 128

        def x_tile(r, t):
            return xg[h, r, :, pl.ds(pl.multiple_of(t * 128, 128), 128)].astype(F32)

        def over_blocks(fn, init):
            def one(r, c):
                for t in range(tiles):
                    c = fn(r, t, c)
                return c
            return lax.fori_loop(0, num_chips, one, init)

        zero = jnp.zeros((rows, 128), F32)
        with scope("norm"):
            total = over_blocks(lambda r, t, c: c + x_tile(r, t), zero)
            mean = jnp.sum(total, axis=1, keepdims=True) * (1.0 / model_dim)

            def add_square(r, t, c):
                d = x_tile(r, t) - mean
                return c + d * d

            sq = jnp.sum(over_blocks(add_square, zero), axis=1, keepdims=True)
            rstd = lax.rsqrt(sq * (1.0 / model_dim) + 1e-5)

            def scaled(r, c):
                base = chip_at(r) * bw
                for t in range(tiles):
                    g = gain[:, pl.ds(pl.multiple_of(base + t * 128, 128), 128)]
                    pick = lax.broadcasted_iota(jnp.int32, g.shape, 0) == l
                    g = jnp.sum(jnp.where(pick, g, 0.0), axis=0, keepdims=True)
                    a_buf[r, :, t * 128:(t + 1) * 128] = ((x_tile(r, t) - mean) * rstd * g).astype(BF16)
                return c

            lax.fori_loop(0, num_chips, scaled, 0)

    def dot_all(lhs, rhs):
        return sum(jnp.dot(a, b, preferred_element_type=F32) for a, b in zip(lhs, rhs))

    def attn_steps(l, h):
        my_rows = pl.ds(pl.multiple_of(h * rows, rows), rows)

        def ln():
            normalise(l, h, g1)

        def qkv_main():
            @pl.when(h == 0)
            def _():
                wait_w(0, 1, 2, 3)

            with scope("mm_qkv"):
                part = dot_all([a_buf[r] for r in range(4)], [w[r] for r in range(4)])
                for t in range(10):
                    qkv[t, my_rows, :] = part[:, t * head_dim:(t + 1) * head_dim].astype(BF16)

            @pl.when(h == 1)
            def _():
                for r in range(4):
                    load(l, "u", 4 + r, r)

        def qkv_rest():
            @pl.when(h == 0)
            def _():
                wait_w(4, 5)

            with scope("mm_qkv2"):
                part = dot_all([a_buf[r] for r in range(4)],
                               [w[4 + r // 2, :, pl.ds((r % 2) * hw, hw)] for r in range(4)])
                for t in range(5):
                    qkv[10 + t, my_rows, :] = part[:, t * head_dim:(t + 1) * head_dim].astype(BF16)

            @pl.when(h == 1)
            def _():
                load(l, "d", 0, 4)
                load(l, "d", 1, 5)

        def attend(static_h):
            keys = pl.ds(0, (static_h + 1) * rows)
            at = pl.ds(static_h * rows, rows)
            shape = (rows, (static_h + 1) * rows)
            q_pos = static_h * rows + lax.broadcasted_iota(jnp.int32, shape, 0)
            keep = lax.broadcasted_iota(jnp.int32, shape, 1) <= q_pos
            scale = 1.0 / math.sqrt(head_dim)

            @pl.when(h == static_h)
            def _():
                with scope("attn"):
                    for n in range(heads):
                        s = lax.dot_general(qkv[3 * n, at, :], qkv[3 * n + 1, keys, :], (((1,), (1,)), ((), ())),
                                            preferred_element_type=F32) * scale
                        s = jnp.where(keep, s, -1e30)
                        p = jnp.exp(s - jnp.max(s, axis=1, keepdims=True))
                        total = jnp.sum(p, axis=1, keepdims=True)
                        mix = jnp.dot(p.astype(BF16), qkv[3 * n + 2, keys, :], preferred_element_type=F32)
                        o_buf[:, n * head_dim:(n + 1) * head_dim] = (mix / total).astype(BF16)

        def attend_both():
            attend(0)
            attend(1)

        def prod(n):
            d = ORDER[n]
            s = 6 + n // 2
            if n % 2 == 0:
                @pl.when(h == 0)
                def _():
                    wait_w(s)

            with scope("mm_out"):
                pb[h, d] = jnp.dot(o_buf[...], w[s, pl.ds((n % 2) * hw, hw), :],
                                   preferred_element_type=F32).astype(BF16)
            send(h, PAIR + d)
            if n % 2 == 1:
                @pl.when(h == 1)
                def _():
                    load(l, "d", 2 + n // 2, s)

        return [ln, qkv_main, qkv_rest, attend_both] + [functools.partial(prod, n) for n in range(4)]

    def mlp_steps(l, h):
        def ln():
            normalise(l, h, g2)

        def up(n):
            base = 8 if n == 0 else 4 * h
            if n == 0:
                @pl.when(h == 0)
                def _():
                    wait_w(8, 9, 10, 11)
            else:
                wait_w(*[base + r for r in range(4)])
            with scope("mm_up"):
                part = dot_all([a_buf[r] for r in range(4)], [w[base + r] for r in range(4)])
                h_buf[:, pl.ds(n * bw, bw)] = jax.nn.gelu(part, approximate=True).astype(BF16)

            @pl.when(h == 1 - n)
            def _():
                for r in range(4):
                    load(l, "d", 4 + r, base + r)

            if n == 1:
                @pl.when(h == 1)
                def _():
                    load_next(l, "q", 4, 4)
                    load_next(l, "q", 5, 5)
                    load_next(l, "o", 0, 6)
                    load_next(l, "o", 1, 7)

        def prod(n):
            d = ORDER[n]
            s0, s1 = ((4, 0), (6, 2), (0, 8), (2, 10))[n]
            s = s0 + h * (s1 - s0)
            wait_w(s, s + 1)
            with scope("mm_down"):
                part = dot_all([h_buf[:, 0:bw], h_buf[:, bw:2 * bw]], [w[s], w[s + 1]])
                pb[h, d] = part.astype(BF16)
            send(h, PAIR + d)

            @pl.when(h == 0)
            def _():
                for i in range(2):
                    if n < 2:
                        load(l, "u", 4 + 2 * n + i, s0 + i)
                    else:
                        load(l, "d", 2 * (n - 2) + i, s0 + i)

            @pl.when(h == 1)
            def _():
                for i in range(2):
                    if n < 2:
                        load_next(l, "q", 2 * n + i, s1 + i)
                    else:
                        load_next(l, "u", 2 * (n - 2) + i, s1 + i)

        return [ln, functools.partial(up, 0), functools.partial(up, 1)] + [
            functools.partial(prod, n) for n in range(4)]

    def run(steps, h, plan, guard):
        g = 1 - h

        def other(events):
            if guard is None:
                for ev in events:
                    ev(g)
            elif events:
                @pl.when(guard)
                def _():
                    for ev in events:
                        ev(g)

        for n, step in enumerate(steps):
            step()
            for whose, events in plan.get(n, ()):
                if whose == OTHER:
                    other(events)
                else:
                    for ev in events:
                        ev(h)

    def x_copy(h, r):
        return pltpu.make_async_copy(x_hbm.at[pl.ds(h * rows, rows), block(r)], xg.at[h, r], xsem.at[h, r])

    def out_copy(h, r):
        return pltpu.make_async_copy(xg.at[h, r], out.at[pl.ds(h * rows, rows), block(r)], xsem.at[h, r])

    for r in range(num_chips):
        x_copy(0, r).start()
    for r in range(4):
        load(0, "q", r, r)
    barrier = pltpu.get_barrier_semaphore()
    for n in range(1, tp):
        pl.semaphore_signal(barrier, inc=1, device_id={"tp": lax.rem(me + n, tp)},
                            device_id_type=pl.DeviceIdType.MESH)
    with scope("xwait"):
        for r in range(num_chips):
            x_copy(0, r).wait()
    for r in range(num_chips):
        x_copy(1, r).start()
    load(0, "q", 4, 4)
    load(0, "q", 5, 5)
    load(0, "o", 0, 6)
    load(0, "o", 1, 7)
    for r in range(4):
        load(0, "u", r, 8 + r)
    with scope("bar"):
        pl.semaphore_wait(barrier, tp - 1)
    for r in range(num_chips):
        x_copy(1, r).wait()

    def layer(l, c):
        def attn_half(h, c):
            run(attn_steps(l, h), h, {
                0: [(OTHER, [ev3])],
                2: [(OTHER, [ev4])],
                6: [(SELF, [ev1])],
                7: [(OTHER, [ev5]), (SELF, [ev2]), (OTHER, [ev6, ev7, ev8])],
            }, l + h > 0)
            return c

        def mlp_half(h, c):
            run(mlp_steps(l, h), h, {
                0: [(OTHER, [ev3])],
                2: [(OTHER, [ev4])],
                4: [(SELF, [ev1])],
                5: [(OTHER, [ev5])],
                6: [(SELF, [ev2]), (OTHER, [ev6, ev7, ev8])],
            }, None)
            return c

        lax.fori_loop(0, 2, attn_half, 0)
        lax.fori_loop(0, 2, mlp_half, 0)
        return c

    lax.fori_loop(0, num_layers, layer, 0)
    ev3(1)
    ev4(1)
    for r in range(num_chips):
        out_copy(0, r).start()
    for ev in (ev5, ev6, ev7, ev8):
        ev(1)
    for r in range(num_chips):
        out_copy(1, r).start()
    with scope("outw"):
        for h in range(2):
            for r in range(num_chips):
                out_copy(h, r).wait()


def solution(mesh):
    tp = mesh.shape["tp"]
    num_chips = tp // 2

    def device_fn(act_in, w_qkv, w_out, w_up, w_down, gain_one, gain_two):
        seq, model_dim = act_in.shape
        num_layers, _, heads, _, head_dim = w_qkv.shape
        ffn = w_up.shape[2]
        bw = model_dim // num_chips
        half, hw = seq // 2, bw // 2
        wq = jnp.transpose(w_qkv, (0, 2, 3, 1, 4)).reshape(num_layers, heads * 3, model_dim, head_dim)
        wo = w_out.reshape(num_layers, heads * head_dim, model_dim)
        vmem = pl.BlockSpec(memory_space=pltpu.VMEM)
        hbm = pl.BlockSpec(memory_space=pl.ANY)
        return pl.pallas_call(
            functools.partial(layer_kernel, num_layers, num_chips, heads, head_dim),
            out_shape=jax.ShapeDtypeStruct((seq, model_dim), BF16),
            in_specs=[hbm] * 5 + [vmem] * 2,
            out_specs=hbm,
            scratch_shapes=[
                pltpu.VMEM((2, num_chips, half, bw), BF16),
                pltpu.VMEM((num_chips, half, bw), BF16),
                pltpu.VMEM((2, num_chips, half, bw), BF16),
                pltpu.VMEM((2, num_chips, half // 2, bw), BF16),
                pltpu.VMEM((2, 6, half // 2, hw), BF16),
                pltpu.VMEM((2, 6, half // 2, hw), BF16),
                pltpu.VMEM((heads * 3, seq, head_dim), BF16),
                pltpu.VMEM((half, heads * head_dim), BF16),
                pltpu.VMEM((half, ffn), BF16),
                pltpu.VMEM((SLOTS, bw, bw), BF16),
                pltpu.SemaphoreType.DMA((SLOTS,)),
                pltpu.SemaphoreType.DMA((2, num_chips)),
                pltpu.SemaphoreType.DMA((2, KINDS)),
                pltpu.SemaphoreType.DMA((2, KINDS)),
            ],
            compiler_params=pltpu.CompilerParams(
                collective_id=0, has_side_effects=True, vmem_limit_bytes=60 * 2 ** 20),
            name="layers",
        )(act_in, wq, wo, w_up, w_down, gain_one, gain_two)

    return jax.shard_map(
        device_fn,
        mesh=mesh,
        in_specs=(
            P("dp", None),
            P(None, None, "tp", None, None),
            P(None, "tp", None, None),
            P(None, None, "tp"),
            P(None, "tp", None),
            P(None, None),
            P(None, None),
        ),
        out_specs=P("dp", None),
        check_vma=False,
    )
```

```python
import functools
import math

import jax
import jax.numpy as jnp
from jax import lax
from jax.experimental import pallas as pl
from jax.experimental.pallas import tpu as pltpu
from jax.sharding import PartitionSpec as P

F32 = jnp.float32
BF16 = jnp.bfloat16
SLOTS = 12
PAIR, M1R, M1L, M2R, M2L, M3R, M3L = 0, 4, 5, 6, 7, 8, 9
OWN_RA, OWN_RB, OWN_LA, OWN_LB, FWD_R, FWD_L = 10, 11, 12, 13, 14, 15
SH_OWN, SH_LA, SH_LB, SH_RA, SH_RB, SH_OA, SH_OB = 16, 17, 18, 19, 20, 21, 22
KINDS = 23
ORDER = (2, 1, 3, 0)
SELF, OTHER = 0, 1


def layer_kernel(
    num_layers, num_chips, heads, head_dim,
    x_hbm, wq, wo, w1, w2, g1, g2, out,
    xg, a_buf, pb, pr, sb, rb, qkv, o_buf, h_buf, gains, w,
    wsem, xsem, ssem, rsem,
):
    rows = xg.shape[2]
    bw = xg.shape[3]
    own = rows // 2
    hw = bw // 2
    model_dim = num_chips * bw
    tp = 2 * num_chips
    me = lax.axis_index("tp")
    chip = me // 2
    core = me % 2
    mine = pl.ds(pl.multiple_of(core * own, own), own)
    theirs = pl.ds(pl.multiple_of((1 - core) * own, own), own)
    scope = jax.named_scope

    def chip_at(r):
        return lax.rem(chip + r, num_chips)

    def block(r):
        return pl.ds(pl.multiple_of(chip_at(r) * bw, bw), bw)

    right = chip_at(1) * 2 + core
    left = chip_at(3) * 2 + core
    partner = chip * 2 + (1 - core)
    half_a = pl.ds(0, hw)
    half_b = pl.ds(hw, hw)

    def load(l, what, n, s):
        res = []

        def slab(t, r, col):
            res.append((wq.at[l, t, block(r), :], w.at[s, :, pl.ds(col, head_dim)]))

        if what == "q" and n < 4:
            for t in range(10):
                slab(t, n, t * head_dim)
        elif what == "q":
            for i in range(2):
                for t in range(5):
                    slab(10 + t, 2 * (n - 4) + i, i * hw + t * head_dim)
        elif what == "o":
            for i in range(2):
                res.append((wo.at[l, :, block(ORDER[2 * n + i])], w.at[s, pl.ds(i * hw, hw), :]))
        elif what == "u":
            res.append((w1.at[l, block(n % 4), pl.ds((n // 4) * bw, bw)], w.at[s]))
        else:
            res.append((w2.at[l, pl.ds((n % 2) * bw, bw), block(ORDER[n // 2])], w.at[s]))
        for a, b in res:
            pltpu.make_async_copy(a, b, wsem.at[s]).start()

    def load_next(l, what, n, s):
        @pl.when(l + 1 < num_layers)
        def _():
            load(l + 1, what, n, s)

    def wait_w(*slots):
        with scope("wwait"):
            for s in slots:
                pltpu.make_async_copy(w.at[s], w.at[s], wsem.at[s]).wait()

    def msg(h, kind):
        def rc(src, dst, dev):
            return pltpu.make_async_remote_copy(
                src_ref=src, dst_ref=dst, send_sem=ssem.at[h, kind], recv_sem=rsem.at[h, kind],
                device_id={"tp": dev}, device_id_type=pl.DeviceIdType.MESH,
            )

        def move(r_from, r_to, cols, dev):
            return rc(xg.at[h, r_from, mine, cols], xg.at[h, r_to, mine, cols], dev)

        if kind < 4:
            return rc(pb.at[h, kind, theirs, :], pr.at[h, kind], partner)
        if kind <= M3L:
            n = kind - M1R
            return rc(sb.at[h, n], rb.at[h, n], right if n % 2 == 0 else left)
        return move(*{
            OWN_RA: (0, 3, half_a, right), OWN_RB: (0, 3, half_b, right),
            OWN_LA: (0, 1, half_a, left), OWN_LB: (0, 1, half_b, left),
            FWD_R: (3, 2, half_a, right), FWD_L: (1, 2, half_b, left),
            SH_OWN: (0, 0, pl.ds(0, bw), partner),
            SH_LA: (3, 3, half_a, partner), SH_LB: (3, 3, half_b, partner),
            SH_RA: (1, 1, half_a, partner), SH_RB: (1, 1, half_b, partner),
            SH_OA: (2, 2, half_a, partner), SH_OB: (2, 2, half_b, partner),
        }[kind])

    def send(h, *kinds):
        for kind in kinds:
            msg(h, kind).start()

    def recv(h, *kinds):
        for kind in kinds:
            with scope("recv%d" % kind):
                msg(h, kind).wait_recv()

    def pair_sum(h, d, cols):
        return pb[h, d, mine, cols].astype(F32) + pr[h, d, :, cols].astype(F32)

    def ev1(h):
        recv(h, PAIR + 2)
        sb[h, 0] = pair_sum(h, 2, half_a).astype(BF16)
        sb[h, 1] = pair_sum(h, 2, half_b).astype(BF16)
        send(h, M1R, M1L)

    def ev2(h):
        recv(h, PAIR + 1)
        sb[h, 2] = pair_sum(h, 1, half_b).astype(BF16)
        recv(h, PAIR + 3)
        sb[h, 3] = pair_sum(h, 3, half_a).astype(BF16)
        send(h, M2R, M2L)

    def ev3(h):
        recv(h, M1R)
        sb[h, 4] = (pair_sum(h, 1, half_a) + rb[h, 0].astype(F32)).astype(BF16)
        send(h, M3R)
        recv(h, M1L)
        sb[h, 5] = (pair_sum(h, 3, half_b) + rb[h, 1].astype(F32)).astype(BF16)
        send(h, M3L)

    def ev4(h):
        recv(h, PAIR + 0, M2L, M3R)
        xg[h, 0, mine, half_a] = (xg[h, 0, mine, half_a].astype(F32) + (
            pair_sum(h, 0, half_a) + rb[h, 3].astype(F32) + rb[h, 4].astype(F32))).astype(BF16)
        send(h, OWN_RA)
        recv(h, M2R, M3L)
        xg[h, 0, mine, half_b] = (xg[h, 0, mine, half_b].astype(F32) + (
            pair_sum(h, 0, half_b) + rb[h, 2].astype(F32) + rb[h, 5].astype(F32))).astype(BF16)
        send(h, OWN_LB, OWN_LA, OWN_RB, SH_OWN)

    def ev5(h):
        recv(h, OWN_RA)
        send(h, FWD_R, SH_LA)
        recv(h, OWN_LB)
        send(h, FWD_L, SH_RB)

    def ev6(h):
        recv(h, OWN_LA)
        send(h, SH_RA)
        recv(h, OWN_RB)
        send(h, SH_LB)

    def ev7(h):
        recv(h, FWD_R)
        send(h, SH_OA)
        recv(h, FWD_L)
        send(h, SH_OB)

    def ev8(h):
        recv(h, SH_OWN, SH_LA, SH_LB, SH_RA, SH_RB, SH_OA, SH_OB)
        with scope("sent"):
            for kind in range(KINDS):
                msg(h, kind).wait_send()

    def normalise(l, h, which):
        tiles = bw // 128

        def x_tile(r, t):
            return xg[h, r, :, pl.ds(pl.multiple_of(t * 128, 128), 128)].astype(F32)

        def over_blocks(fn, init):
            def one(r, c):
                for t in range(tiles):
                    c = fn(r, t, c)
                return c
            return lax.fori_loop(0, num_chips, one, init)

        zero = jnp.zeros((rows, 128), F32)
        with scope("norm"):
            total = over_blocks(lambda r, t, c: c + x_tile(r, t), zero)
            mean = jnp.sum(total, axis=1, keepdims=True) * (1.0 / model_dim)

            def add_square(r, t, c):
                d = x_tile(r, t) - mean
                return c + d * d

            sq = jnp.sum(over_blocks(add_square, zero), axis=1, keepdims=True)
            rstd = lax.rsqrt(sq * (1.0 / model_dim) + 1e-5)

            def scaled(r, c):
                for t in range(tiles):
                    g = gains[which, l, r, :, t * 128:(t + 1) * 128]
                    a_buf[r, :, t * 128:(t + 1) * 128] = ((x_tile(r, t) - mean) * rstd * g).astype(BF16)
                return c

            lax.fori_loop(0, num_chips, scaled, 0)

    def dot_all(lhs, rhs):
        return sum(jnp.dot(a, b, preferred_element_type=F32) for a, b in zip(lhs, rhs))

    def attn_steps(l, h):
        my_rows = pl.ds(pl.multiple_of(h * rows, rows), rows)

        def ln():
            normalise(l, h, 0)

            @pl.when(l + h == 0)
            def _():
                load(0, "q", 4, 4)
                load(0, "q", 5, 5)
                load(0, "o", 0, 6)
                load(0, "o", 1, 7)

        def qkv_main():
            @pl.when(h == 0)
            def _():
                wait_w(0, 1, 2, 3)

            with scope("mm_qkv"):
                part = dot_all([a_buf[r] for r in range(4)], [w[r] for r in range(4)])
                for t in range(10):
                    qkv[t, my_rows, :] = part[:, t * head_dim:(t + 1) * head_dim].astype(BF16)

            @pl.when(h == 1)
            def _():
                for r in range(4):
                    load(l, "u", 4 + r, r)

            @pl.when(l + h == 0)
            def _():
                for r in range(4):
                    load(0, "u", r, 8 + r)

        def qkv_rest():
            @pl.when(h == 0)
            def _():
                wait_w(4, 5)

            with scope("mm_qkv2"):
                part = dot_all([a_buf[r] for r in range(4)],
                               [w[4 + r // 2, :, pl.ds((r % 2) * hw, hw)] for r in range(4)])
                for t in range(5):
                    qkv[10 + t, my_rows, :] = part[:, t * head_dim:(t + 1) * head_dim].astype(BF16)

            @pl.when(h == 1)
            def _():
                load(l, "d", 0, 4)
                load(l, "d", 1, 5)

        def attend():
            shape = (rows, 2 * rows)
            q_pos = h * rows + lax.broadcasted_iota(jnp.int32, shape, 0)
            keep = lax.broadcasted_iota(jnp.int32, shape, 1) <= q_pos
            scale = 1.0 / math.sqrt(head_dim)
            with scope("attn"):
                for n in range(heads):
                    s = lax.dot_general(qkv[3 * n, my_rows, :], qkv[3 * n + 1], (((1,), (1,)), ((), ())),
                                        preferred_element_type=F32) * scale
                    s = jnp.where(keep, s, -1e30)
                    p = jnp.exp(s - jnp.max(s, axis=1, keepdims=True))
                    total = jnp.sum(p, axis=1, keepdims=True)
                    mix = jnp.dot(p.astype(BF16), qkv[3 * n + 2], preferred_element_type=F32)
                    o_buf[:, n * head_dim:(n + 1) * head_dim] = (mix / total).astype(BF16)

        def prod(n):
            d = ORDER[n]
            s = 6 + n // 2
            if n % 2 == 0:
                @pl.when(h == 0)
                def _():
                    wait_w(s)

            with scope("mm_out"):
                pb[h, d] = jnp.dot(o_buf[...], w[s, pl.ds((n % 2) * hw, hw), :],
                                   preferred_element_type=F32).astype(BF16)
            send(h, PAIR + d)
            if n % 2 == 1:
                @pl.when(h == 1)
                def _():
                    load(l, "d", 2 + n // 2, s)

        return [ln, qkv_main, qkv_rest, attend] + [functools.partial(prod, n) for n in range(4)]

    def mlp_steps(l, h):
        def ln():
            normalise(l, h, 1)

        def up(n):
            base = 8 if n == 0 else 4 * h
            if n == 0:
                @pl.when(h == 0)
                def _():
                    wait_w(8, 9, 10, 11)
            else:
                wait_w(*[base + r for r in range(4)])
            with scope("mm_up"):
                part = dot_all([a_buf[r] for r in range(4)], [w[base + r] for r in range(4)])
                h_buf[:, pl.ds(n * bw, bw)] = jax.nn.gelu(part, approximate=True).astype(BF16)

            @pl.when(h == 1 - n)
            def _():
                for r in range(4):
                    load(l, "d", 4 + r, base + r)

            if n == 1:
                @pl.when(h == 1)
                def _():
                    load_next(l, "q", 4, 4)
                    load_next(l, "q", 5, 5)
                    load_next(l, "o", 0, 6)
                    load_next(l, "o", 1, 7)

        def prod(n):
            d = ORDER[n]
            s0, s1 = ((4, 0), (6, 2), (0, 8), (2, 10))[n]
            s = s0 + h * (s1 - s0)
            wait_w(s, s + 1)
            with scope("mm_down"):
                part = dot_all([h_buf[:, 0:bw], h_buf[:, bw:2 * bw]], [w[s], w[s + 1]])
                pb[h, d] = part.astype(BF16)
            send(h, PAIR + d)

            @pl.when(h == 0)
            def _():
                for i in range(2):
                    if n < 2:
                        load(l, "u", 4 + 2 * n + i, s0 + i)
                    else:
                        load(l, "d", 2 * (n - 2) + i, s0 + i)

            @pl.when(h == 1)
            def _():
                for i in range(2):
                    if n < 2:
                        load_next(l, "q", 2 * n + i, s1 + i)
                    else:
                        load_next(l, "u", 2 * (n - 2) + i, s1 + i)

        return [ln, functools.partial(up, 0), functools.partial(up, 1)] + [
            functools.partial(prod, n) for n in range(4)]

    def run(steps, h, plan, guard):
        g = 1 - h

        def other(events):
            if guard is None:
                for ev in events:
                    ev(g)
            elif events:
                @pl.when(guard)
                def _():
                    for ev in events:
                        ev(g)

        for n, step in enumerate(steps):
            step()
            for whose, events in plan.get(n, ()):
                if whose == OTHER:
                    other(events)
                else:
                    for ev in events:
                        ev(h)

    def x_copy(h, r):
        return pltpu.make_async_copy(x_hbm.at[pl.ds(h * rows, rows), block(r)], xg.at[h, r], xsem.at[h, r])

    def out_copy(h, r):
        return pltpu.make_async_copy(xg.at[h, r], out.at[pl.ds(h * rows, rows), block(r)], xsem.at[h, r])

    for h in range(2):
        for r in range(num_chips):
            x_copy(h, r).start()
    load(0, "q", 0, 0)
    barrier = pltpu.get_barrier_semaphore()
    for n in range(1, tp):
        pl.semaphore_signal(barrier, inc=1, device_id={"tp": lax.rem(me + n, tp)},
                            device_id_type=pl.DeviceIdType.MESH)
    qkv[...] = jnp.zeros_like(qkv)
    for k, gain in enumerate((g1, g2)):
        for l in range(num_layers):
            for r in range(num_chips):
                gains[k, l, r] = gain[pl.ds(l, 1), block(r)]
    with scope("xwait"):
        for h in range(2):
            for r in range(num_chips):
                x_copy(h, r).wait()
    for r in range(1, 4):
        load(0, "q", r, r)
    with scope("bar"):
        pl.semaphore_wait(barrier, tp - 1)

    def layer(l, c):
        def attn_half(h, c):
            run(attn_steps(l, h), h, {
                1: [(OTHER, [ev4])],
                3: [(OTHER, [ev5])],
                5: [(SELF, [ev1]), (OTHER, [ev6])],
                6: [(OTHER, [ev7])],
                7: [(SELF, [ev2]), (OTHER, [ev8]), (SELF, [ev3])],
            }, l + h > 0)
            return c

        def mlp_half(h, c):
            run(mlp_steps(l, h), h, {
                1: [(OTHER, [ev4])],
                2: [(OTHER, [ev5])],
                3: [(OTHER, [ev6])],
                4: [(SELF, [ev1])],
                5: [(OTHER, [ev7])],
                6: [(SELF, [ev2, ev3]), (OTHER, [ev8])],
            }, None)
            return c

        lax.fori_loop(0, 2, attn_half, 0)
        lax.fori_loop(0, 2, mlp_half, 0)
        return c

    lax.fori_loop(0, num_layers, layer, 0)
    ev4(1)
    for r in range(num_chips):
        out_copy(0, r).start()
    for ev in (ev5, ev6, ev7, ev8):
        ev(1)
    for r in range(num_chips):
        out_copy(1, r).start()
    with scope("outw"):
        for h in range(2):
            for r in range(num_chips):
                out_copy(h, r).wait()


def solution(mesh):
    tp = mesh.shape["tp"]
    num_chips = tp // 2

    def device_fn(act_in, w_qkv, w_out, w_up, w_down, gain_one, gain_two):
        seq, model_dim = act_in.shape
        num_layers, _, heads, _, head_dim = w_qkv.shape
        ffn = w_up.shape[2]
        bw = model_dim // num_chips
        half, hw = seq // 2, bw // 2
        wq = jnp.transpose(w_qkv, (0, 2, 3, 1, 4)).reshape(num_layers, heads * 3, model_dim, head_dim)
        wo = w_out.reshape(num_layers, heads * head_dim, model_dim)
        vmem = pl.BlockSpec(memory_space=pltpu.VMEM)
        hbm = pl.BlockSpec(memory_space=pl.ANY)
        return pl.pallas_call(
            functools.partial(layer_kernel, num_layers, num_chips, heads, head_dim),
            out_shape=jax.ShapeDtypeStruct((seq, model_dim), BF16),
            in_specs=[hbm] * 5 + [vmem] * 2,
            out_specs=hbm,
            scratch_shapes=[
                pltpu.VMEM((2, num_chips, half, bw), BF16),
                pltpu.VMEM((num_chips, half, bw), BF16),
                pltpu.VMEM((2, num_chips, half, bw), BF16),
                pltpu.VMEM((2, num_chips, half // 2, bw), BF16),
                pltpu.VMEM((2, 6, half // 2, hw), BF16),
                pltpu.VMEM((2, 6, half // 2, hw), BF16),
                pltpu.VMEM((heads * 3, seq, head_dim), BF16),
                pltpu.VMEM((half, heads * head_dim), BF16),
                pltpu.VMEM((half, ffn), BF16),
                pltpu.VMEM((2, num_layers, num_chips, 1, bw), F32),
                pltpu.VMEM((SLOTS, bw, bw), BF16),
                pltpu.SemaphoreType.DMA((SLOTS,)),
                pltpu.SemaphoreType.DMA((2, num_chips)),
                pltpu.SemaphoreType.DMA((2, KINDS)),
                pltpu.SemaphoreType.DMA((2, KINDS)),
            ],
            compiler_params=pltpu.CompilerParams(
                collective_id=0, has_side_effects=True, vmem_limit_bytes=54 * 2 ** 20),
            name="layers",
        )(act_in, wq, wo, w_up, w_down, gain_one, gain_two)

    return jax.shard_map(
        device_fn,
        mesh=mesh,
        in_specs=(
            P("dp", None),
            P(None, None, "tp", None, None),
            P(None, "tp", None, None),
            P(None, None, "tp"),
            P(None, "tp", None),
            P(None, None),
            P(None, None),
        ),
        out_specs=P("dp", None),
        check_vma=False,
    )
```

```python
import functools
import math

import jax
import jax.numpy as jnp
from jax import lax
from jax.experimental import pallas as pl
from jax.experimental.pallas import tpu as pltpu
from jax.sharding import PartitionSpec as P

F32 = jnp.float32
BF16 = jnp.bfloat16
SLOTS = 12
PAIR, M1R, M1L, M2R, M2L, M3R, M3L = 0, 4, 5, 6, 7, 8, 9
OWN_RA, OWN_RB, OWN_LA, OWN_LB, FWD_R, FWD_L = 10, 11, 12, 13, 14, 15
SH_OWN, SH_LA, SH_LB, SH_RA, SH_RB, SH_OA, SH_OB = 16, 17, 18, 19, 20, 21, 22
KINDS = 23
ORDER = (2, 3, 1, 0)
SELF, OTHER = 0, 1


def layer_kernel(
    num_layers, num_chips, heads, head_dim,
    x_hbm, wq, wo, w1, w2, g1, g2, out,
    xg, a_buf, pb, pr, sb, rb, qkv, o_buf, h_buf, gains, w,
    wsem, xsem, ssem, rsem,
):
    rows = xg.shape[2]
    bw = xg.shape[3]
    own = rows // 2
    hw = bw // 2
    model_dim = num_chips * bw
    tp = 2 * num_chips
    me = lax.axis_index("tp")
    chip = me // 2
    core = me % 2
    mine = pl.ds(pl.multiple_of(core * own, own), own)
    theirs = pl.ds(pl.multiple_of((1 - core) * own, own), own)
    scope = jax.named_scope

    def chip_at(r):
        return lax.rem(chip + r, num_chips)

    def block(r):
        return pl.ds(pl.multiple_of(chip_at(r) * bw, bw), bw)

    right = chip_at(1) * 2 + core
    left = chip_at(3) * 2 + core
    partner = chip * 2 + (1 - core)
    half_a = pl.ds(0, hw)
    half_b = pl.ds(hw, hw)

    def load(l, what, n, s):
        res = []

        def slab(t, r, col):
            res.append((wq.at[l, t, block(r), :], w.at[s, :, pl.ds(col, head_dim)]))

        if what == "q" and n < 4:
            for t in range(10):
                slab(t, n, t * head_dim)
        elif what == "q":
            for i in range(2):
                for t in range(5):
                    slab(10 + t, 2 * (n - 4) + i, i * hw + t * head_dim)
        elif what == "o":
            for i in range(2):
                res.append((wo.at[l, :, block(ORDER[2 * n + i])], w.at[s, pl.ds(i * hw, hw), :]))
        elif what == "u":
            res.append((w1.at[l, block(n % 4), pl.ds((n // 4) * bw, bw)], w.at[s]))
        else:
            res.append((w2.at[l, pl.ds((n % 2) * bw, bw), block(ORDER[n // 2])], w.at[s]))
        for a, b in res:
            pltpu.make_async_copy(a, b, wsem.at[s]).start()

    def load_next(l, what, n, s):
        @pl.when(l + 1 < num_layers)
        def _():
            load(l + 1, what, n, s)

    def wait_w(*slots):
        with scope("wwait"):
            for s in slots:
                pltpu.make_async_copy(w.at[s], w.at[s], wsem.at[s]).wait()

    def msg(h, kind):
        def rc(src, dst, dev):
            return pltpu.make_async_remote_copy(
                src_ref=src, dst_ref=dst, send_sem=ssem.at[h, kind], recv_sem=rsem.at[h, kind],
                device_id={"tp": dev}, device_id_type=pl.DeviceIdType.MESH,
            )

        def move(r_from, r_to, cols, dev):
            return rc(xg.at[h, r_from, mine, cols], xg.at[h, r_to, mine, cols], dev)

        if kind < 4:
            return rc(pb.at[h, kind, theirs, :], pr.at[h, kind], partner)
        if kind <= M3L:
            n = kind - M1R
            return rc(sb.at[h, n], rb.at[h, n], right if n % 2 == 0 else left)
        return move(*{
            OWN_RA: (0, 3, half_a, right), OWN_RB: (0, 3, half_b, right),
            OWN_LA: (0, 1, half_a, left), OWN_LB: (0, 1, half_b, left),
            FWD_R: (3, 2, half_a, right), FWD_L: (1, 2, half_b, left),
            SH_OWN: (0, 0, pl.ds(0, bw), partner),
            SH_LA: (3, 3, half_a, partner), SH_LB: (3, 3, half_b, partner),
            SH_RA: (1, 1, half_a, partner), SH_RB: (1, 1, half_b, partner),
            SH_OA: (2, 2, half_a, partner), SH_OB: (2, 2, half_b, partner),
        }[kind])

    def send_pair(h, d):
        pltpu.make_async_remote_copy(
            src_ref=pb.at[h, d, theirs, :], dst_ref=pr.at[h, d], send_sem=ssem.at[h, d], recv_sem=rsem.at[h, d],
            device_id={"tp": partner}, device_id_type=pl.DeviceIdType.MESH,
        ).start()

    def send(h, *kinds):
        for kind in kinds:
            msg(h, kind).start()

    def recv(h, *kinds):
        for kind in kinds:
            with scope("recv%d" % kind):
                msg(h, kind).wait_recv()

    def pair_sum(h, d, cols):
        return pb[h, d, mine, cols].astype(F32) + pr[h, d, :, cols].astype(F32)

    def ev1(h):
        recv(h, PAIR + 2)
        sb[h, 0] = pair_sum(h, 2, half_a).astype(BF16)
        sb[h, 1] = pair_sum(h, 2, half_b).astype(BF16)
        send(h, M1R, M1L)

    def ev2(h):
        recv(h, PAIR + 1)
        sb[h, 2] = pair_sum(h, 1, half_b).astype(BF16)
        recv(h, PAIR + 3)
        sb[h, 3] = pair_sum(h, 3, half_a).astype(BF16)
        send(h, M2R, M2L)

    def ev3(h):
        recv(h, M1R)
        sb[h, 4] = (pair_sum(h, 1, half_a) + rb[h, 0].astype(F32)).astype(BF16)
        send(h, M3R)
        recv(h, M1L)
        sb[h, 5] = (pair_sum(h, 3, half_b) + rb[h, 1].astype(F32)).astype(BF16)
        send(h, M3L)

    def ev4(h):
        recv(h, PAIR + 0, M2L, M3R)
        xg[h, 0, mine, half_a] = (xg[h, 0, mine, half_a].astype(F32) + (
            pair_sum(h, 0, half_a) + rb[h, 3].astype(F32) + rb[h, 4].astype(F32))).astype(BF16)
        send(h, OWN_RA)
        recv(h, M2R, M3L)
        xg[h, 0, mine, half_b] = (xg[h, 0, mine, half_b].astype(F32) + (
            pair_sum(h, 0, half_b) + rb[h, 2].astype(F32) + rb[h, 5].astype(F32))).astype(BF16)
        send(h, OWN_LB, OWN_LA, OWN_RB, SH_OWN)

    def ev5(h):
        recv(h, OWN_RA)
        send(h, FWD_R, SH_LA)
        recv(h, OWN_LB)
        send(h, FWD_L, SH_RB)

    def ev6(h):
        recv(h, OWN_LA)
        send(h, SH_RA)
        recv(h, OWN_RB)
        send(h, SH_LB)

    def ev7(h):
        recv(h, FWD_R)
        send(h, SH_OA)
        recv(h, FWD_L)
        send(h, SH_OB)

    def ev8(h):
        recv(h, SH_OWN, SH_LA, SH_LB, SH_RA, SH_RB, SH_OA, SH_OB)
        with scope("sent"):
            for kind in range(KINDS):
                msg(h, kind).wait_send()

    def normalise(l, h, which):
        tiles = bw // 128

        def x_tile(r, t):
            return xg[h, r, :, pl.ds(pl.multiple_of(t * 128, 128), 128)].astype(F32)

        def over_blocks(fn, init):
            def one(r, c):
                for t in range(tiles):
                    c = fn(r, t, c)
                return c
            return lax.fori_loop(0, num_chips, one, init)

        zero = jnp.zeros((rows, 128), F32)
        with scope("norm"):
            total = over_blocks(lambda r, t, c: c + x_tile(r, t), zero)
            mean = jnp.sum(total, axis=1, keepdims=True) * (1.0 / model_dim)

            def add_square(r, t, c):
                d = x_tile(r, t) - mean
                return c + d * d

            sq = jnp.sum(over_blocks(add_square, zero), axis=1, keepdims=True)
            rstd = lax.rsqrt(sq * (1.0 / model_dim) + 1e-5)

            def scaled(r, c):
                for t in range(tiles):
                    g = gains[which, l, r, :, t * 128:(t + 1) * 128]
                    a_buf[r, :, t * 128:(t + 1) * 128] = ((x_tile(r, t) - mean) * rstd * g).astype(BF16)
                return c

            lax.fori_loop(0, num_chips, scaled, 0)

    def dot_all(lhs, rhs):
        return sum(jnp.dot(a, b, preferred_element_type=F32) for a, b in zip(lhs, rhs))

    def attn_steps(l, h):
        my_rows = pl.ds(pl.multiple_of(h * rows, rows), rows)

        def ln():
            normalise(l, h, 0)

            @pl.when(l + h == 0)
            def _():
                load(0, "q", 4, 4)
                load(0, "q", 5, 5)
                load(0, "o", 0, 6)
                load(0, "o", 1, 7)

        def qkv_main():
            @pl.when(h == 0)
            def _():
                wait_w(0, 1, 2, 3)

            with scope("mm_qkv"):
                part = dot_all([a_buf[r] for r in range(4)], [w[r] for r in range(4)])
                for t in range(10):
                    qkv[t, my_rows, :] = part[:, t * head_dim:(t + 1) * head_dim].astype(BF16)

            @pl.when(h == 1)
            def _():
                for r in range(4):
                    load(l, "u", 4 + r, r)

            @pl.when(l + h == 0)
            def _():
                for r in range(4):
                    load(0, "u", r, 8 + r)

        def qkv_rest():
            @pl.when(h == 0)
            def _():
                wait_w(4, 5)

            with scope("mm_qkv2"):
                part = dot_all([a_buf[r] for r in range(4)],
                               [w[4 + r // 2, :, pl.ds((r % 2) * hw, hw)] for r in range(4)])
                for t in range(5):
                    qkv[10 + t, my_rows, :] = part[:, t * head_dim:(t + 1) * head_dim].astype(BF16)

            @pl.when(h == 1)
            def _():
                load(l, "d", 0, 4)
                load(l, "d", 1, 5)

        def attend_half(static_h):
            at = pl.ds(static_h * rows, rows)
            shape = (rows, 2 * rows)
            q_pos = static_h * rows + lax.broadcasted_iota(jnp.int32, shape, 0)
            keep = lax.broadcasted_iota(jnp.int32, shape, 1) <= q_pos
            scale = 1.0 / math.sqrt(head_dim)
            with scope("attn"):
                for n in range(heads):
                    s = lax.dot_general(qkv[3 * n, at, :], qkv[3 * n + 1], (((1,), (1,)), ((), ())),
                                        preferred_element_type=F32) * scale
                    s = jnp.where(keep, s, -1e30)
                    p = jnp.exp(s - jnp.max(s, axis=1, keepdims=True))
                    total = jnp.sum(p, axis=1, keepdims=True)
                    mix = jnp.dot(p.astype(BF16), qkv[3 * n + 2], preferred_element_type=F32)
                    o_buf[:, n * head_dim:(n + 1) * head_dim] = (mix / total).astype(BF16)

        def attend():
            for static_h in range(2):
                pl.when(h == static_h)(functools.partial(attend_half, static_h))

        def prod(n):
            d = ORDER[n]
            s = 6 + n // 2
            if n % 2 == 0:
                @pl.when(h == 0)
                def _():
                    wait_w(s)

            with scope("mm_out"):
                pb[h, d] = jnp.dot(o_buf[...], w[s, pl.ds((n % 2) * hw, hw), :],
                                   preferred_element_type=F32).astype(BF16)
            send(h, PAIR + d)
            if n % 2 == 1:
                @pl.when(h == 1)
                def _():
                    load(l, "d", 2 + n // 2, s)

        return [ln, qkv_main, qkv_rest, attend] + [functools.partial(prod, n) for n in range(4)]

    def mlp_steps(l, h):
        def ln():
            normalise(l, h, 1)

        def up(n):
            base = 8 + n * (4 * h - 8)

            @pl.when((h == 0) | (n == 1))
            def _():
                wait_w(*[base + r for r in range(4)])

            with scope("mm_up"):
                part = dot_all([a_buf[r] for r in range(4)], [w[base + r] for r in range(4)])
                h_buf[n] = jax.nn.gelu(part, approximate=True).astype(BF16)

            @pl.when(h == 1 - n)
            def _():
                for r in range(4):
                    load(l, "d", 4 + r, base + r)

            @pl.when(h * n == 1)
            def _():
                load_next(l, "q", 4, 4)
                load_next(l, "q", 5, 5)
                load_next(l, "o", 0, 6)
                load_next(l, "o", 1, 7)

        def prod(n):
            d = 2 + n + (n // 2) * (1 - 2 * n)
            s0 = lax.rem(4 + 2 * n, 8)
            s1 = 2 * n + 4 * (n // 2)
            s = s0 + h * (s1 - s0)
            wait_w(s, s + 1)
            with scope("mm_down"):
                part = dot_all([h_buf[0], h_buf[1]], [w[s], w[s + 1]])
                pb[h, d] = part.astype(BF16)
            send_pair(h, d)
            for k in range(4):
                for i in range(2):
                    @pl.when((n == k) & (h == 0))
                    def _():
                        if k < 2:
                            load(l, "u", 4 + 2 * k + i, s0 + i)
                        else:
                            load(l, "d", 2 * (k - 2) + i, s0 + i)

                    @pl.when((n == k) & (h == 1))
                    def _():
                        if k < 2:
                            load_next(l, "q", 2 * k + i, s1 + i)
                        else:
                            load_next(l, "u", 2 * (k - 2) + i, s1 + i)

        return ln, up, prod

    def run_attn(l, h, plan):
        for n, step in enumerate(attn_steps(l, h)):
            step()
            for whose, ev in plan.get(n, ()):
                if whose == SELF:
                    ev(h)
                else:
                    pl.when(l + h > 0)(functools.partial(ev, 1 - h))

    def run_mlp(l, h, plan):
        ln, up, prod = mlp_steps(l, h)

        def events(n, k, at):
            for whose, ev in plan.get(at, ()):
                pl.when(n == k)(functools.partial(ev, h if whose == SELF else 1 - h))

        def up_step(n, c):
            up(n)
            for k in range(2):
                events(n, k, 1 + k)
            return c

        def prod_step(n, c):
            prod(n)
            for k in range(3):
                events(n, k, 3 + k)
            return c

        ln()
        lax.fori_loop(0, 2, up_step, 0)
        lax.fori_loop(0, num_chips, prod_step, 0)
        for whose, ev in plan[6]:
            ev(h if whose == SELF else 1 - h)

    def x_copy(h, r):
        return pltpu.make_async_copy(x_hbm.at[pl.ds(h * rows, rows), block(r)], xg.at[h, r], xsem.at[h, r])

    def out_copy(h, r):
        return pltpu.make_async_copy(xg.at[h, r], out.at[pl.ds(h * rows, rows), block(r)], xsem.at[h, r])

    for h in range(2):
        for r in range(num_chips):
            x_copy(h, r).start()
    load(0, "q", 0, 0)
    barrier = pltpu.get_barrier_semaphore()
    for n in range(1, tp):
        pl.semaphore_signal(barrier, inc=1, device_id={"tp": lax.rem(me + n, tp)},
                            device_id_type=pl.DeviceIdType.MESH)
    qkv[...] = jnp.zeros_like(qkv)
    for k, gain in enumerate((g1, g2)):
        for l in range(num_layers):
            for r in range(num_chips):
                gains[k, l, r] = gain[pl.ds(l, 1), block(r)]
    with scope("xwait"):
        for h in range(2):
            for r in range(num_chips):
                x_copy(h, r).wait()
    for r in range(1, 4):
        load(0, "q", r, r)
    with scope("bar"):
        pl.semaphore_wait(barrier, tp - 1)

    def layer(l, c):
        def attn_half(h, c):
            run_attn(l, h, {
                1: [(OTHER, ev4)],
                5: [(OTHER, ev5)],
                6: [(SELF, ev1), (OTHER, ev6)],
                7: [(SELF, ev2), (OTHER, ev7), (OTHER, ev8), (SELF, ev3)],
            })
            return c

        def mlp_half(h, c):
            run_mlp(l, h, {
                1: [(OTHER, ev4)],
                3: [(OTHER, ev5)],
                4: [(SELF, ev1)],
                5: [(OTHER, ev6)],
                6: [(SELF, ev2), (OTHER, ev7), (SELF, ev3), (OTHER, ev8)],
            })
            return c

        lax.fori_loop(0, 2, attn_half, 0)
        lax.fori_loop(0, 2, mlp_half, 0)
        return c

    lax.fori_loop(0, num_layers, layer, 0)
    ev4(1)
    for r in range(num_chips):
        out_copy(0, r).start()
    for ev in (ev5, ev6, ev7, ev8):
        ev(1)
    for r in range(num_chips):
        out_copy(1, r).start()
    with scope("outw"):
        for h in range(2):
            for r in range(num_chips):
                out_copy(h, r).wait()


def solution(mesh):
    tp = mesh.shape["tp"]
    num_chips = tp // 2

    def device_fn(act_in, w_qkv, w_out, w_up, w_down, gain_one, gain_two):
        seq, model_dim = act_in.shape
        num_layers, _, heads, _, head_dim = w_qkv.shape
        ffn = w_up.shape[2]
        bw = model_dim // num_chips
        half, hw = seq // 2, bw // 2
        wq = jnp.transpose(w_qkv, (0, 2, 3, 1, 4)).reshape(num_layers, heads * 3, model_dim, head_dim)
        wo = w_out.reshape(num_layers, heads * head_dim, model_dim)
        vmem = pl.BlockSpec(memory_space=pltpu.VMEM)
        hbm = pl.BlockSpec(memory_space=pl.ANY)
        return pl.pallas_call(
            functools.partial(layer_kernel, num_layers, num_chips, heads, head_dim),
            out_shape=jax.ShapeDtypeStruct((seq, model_dim), BF16),
            in_specs=[hbm] * 5 + [vmem] * 2,
            out_specs=hbm,
            scratch_shapes=[
                pltpu.VMEM((2, num_chips, half, bw), BF16),
                pltpu.VMEM((num_chips, half, bw), BF16),
                pltpu.VMEM((2, num_chips, half, bw), BF16),
                pltpu.VMEM((2, num_chips, half // 2, bw), BF16),
                pltpu.VMEM((2, 6, half // 2, hw), BF16),
                pltpu.VMEM((2, 6, half // 2, hw), BF16),
                pltpu.VMEM((heads * 3, seq, head_dim), BF16),
                pltpu.VMEM((half, heads * head_dim), BF16),
                pltpu.VMEM((ffn // bw, half, bw), BF16),
                pltpu.VMEM((2, num_layers, num_chips, 1, bw), F32),
                pltpu.VMEM((SLOTS, bw, bw), BF16),
                pltpu.SemaphoreType.DMA((SLOTS,)),
                pltpu.SemaphoreType.DMA((2, num_chips)),
                pltpu.SemaphoreType.DMA((2, KINDS)),
                pltpu.SemaphoreType.DMA((2, KINDS)),
            ],
            compiler_params=pltpu.CompilerParams(
                collective_id=0, has_side_effects=True, vmem_limit_bytes=54 * 2 ** 20),
            name="layers",
        )(act_in, wq, wo, w_up, w_down, gain_one, gain_two)

    return jax.shard_map(
        device_fn,
        mesh=mesh,
        in_specs=(
            P("dp", None),
            P(None, None, "tp", None, None),
            P(None, "tp", None, None),
            P(None, None, "tp"),
            P(None, "tp", None),
            P(None, None),
            P(None, None),
        ),
        out_specs=P("dp", None),
        check_vma=False,
    )
```

```python
import functools
import math

import jax
import jax.numpy as jnp
from jax import lax
from jax.experimental import pallas as pl
from jax.experimental.pallas import tpu as pltpu
from jax.sharding import PartitionSpec as P

F32 = jnp.float32
BF16 = jnp.bfloat16
SLOTS = 12
PAIR, M1R, M1L, M2R, M2L, M3R, M3L = 0, 4, 5, 6, 7, 8, 9
OWN_RA, OWN_RB, OWN_LA, OWN_LB, FWD_R, FWD_L = 10, 11, 12, 13, 14, 15
SH_OWN, SH_LA, SH_LB, SH_RA, SH_RB, SH_OA, SH_OB = 16, 17, 18, 19, 20, 21, 22
KINDS = 23
ORDER = (2, 3, 1, 0)
SPLIT = (M1R, M1L, M3R, M3L, OWN_RA, OWN_LB, FWD_R, FWD_L, SH_OA, SH_OB)
SELF, OTHER = 0, 1


def layer_kernel(
    num_layers, num_chips, heads, head_dim,
    x_hbm, wq, wo, w1, w2, g1, g2, out,
    xg, a_buf, pb, pr, sb, rb, qkv, o_buf, h_buf, gains, w,
    wsem, xsem, ssem, rsem,
):
    rows = xg.shape[2]
    bw = xg.shape[3]
    own = rows // 2
    hw = bw // 2
    model_dim = num_chips * bw
    tp = 2 * num_chips
    me = lax.axis_index("tp")
    chip = me // 2
    core = me % 2
    mine = pl.ds(pl.multiple_of(core * own, own), own)
    theirs = pl.ds(pl.multiple_of((1 - core) * own, own), own)
    scope = jax.named_scope

    def chip_at(r):
        return lax.rem(chip + r, num_chips)

    def block(r):
        return pl.ds(pl.multiple_of(chip_at(r) * bw, bw), bw)

    right = chip_at(1) * 2 + core
    left = chip_at(3) * 2 + core
    partner = chip * 2 + (1 - core)
    half_a = pl.ds(0, hw)
    half_b = pl.ds(hw, hw)

    def load(l, what, n, s):
        res = []

        def slab(t, r, col):
            res.append((wq.at[l, t, block(r), :], w.at[s, :, pl.ds(col, head_dim)]))

        if what == "q" and n < 4:
            for t in range(10):
                slab(t, n, t * head_dim)
        elif what == "q":
            for i in range(2):
                for t in range(5):
                    slab(10 + t, 2 * (n - 4) + i, i * hw + t * head_dim)
        elif what == "o":
            for i in range(2):
                res.append((wo.at[l, :, block(ORDER[2 * n + i])], w.at[s, pl.ds(i * hw, hw), :]))
        elif what == "u":
            res.append((w1.at[l, block(n % 4), pl.ds((n // 4) * bw, bw)], w.at[s]))
        else:
            res.append((w2.at[l, pl.ds((n % 2) * bw, bw), block(ORDER[n // 2])], w.at[s]))
        for a, b in res:
            pltpu.make_async_copy(a, b, wsem.at[s]).start()

    def load_next(l, what, n, s):
        @pl.when(l + 1 < num_layers)
        def _():
            load(l + 1, what, n, s)

    def wait_w(*slots):
        with scope("wwait"):
            for s in slots:
                pltpu.make_async_copy(w.at[s], w.at[s], wsem.at[s]).wait()

    part = own // 2

    def piece(p):
        return pl.ds(0, own) if p is None else pl.ds(p * part, part)

    def mine_of(p):
        return mine if p is None else pl.ds(pl.multiple_of(core * own + p * part, part), part)

    def msg(h, kind, p=None):
        n = 0 if p is None else p

        def rc(src, dst, dev):
            return pltpu.make_async_remote_copy(
                src_ref=src, dst_ref=dst, send_sem=ssem.at[h, kind, n], recv_sem=rsem.at[h, kind, n],
                device_id={"tp": dev}, device_id_type=pl.DeviceIdType.MESH,
            )

        def move(r_from, r_to, cols, dev):
            return rc(xg.at[h, r_from, mine_of(p), cols], xg.at[h, r_to, mine_of(p), cols], dev)

        if kind < 4:
            return rc(pb.at[h, kind, theirs, :], pr.at[h, kind], partner)
        if kind <= M3L:
            k = kind - M1R
            return rc(sb.at[h, k, piece(p), :], rb.at[h, k, piece(p), :], right if k % 2 == 0 else left)
        return move(*{
            OWN_RA: (0, 3, half_a, right), OWN_RB: (0, 3, half_b, right),
            OWN_LA: (0, 1, half_a, left), OWN_LB: (0, 1, half_b, left),
            FWD_R: (3, 2, half_a, right), FWD_L: (1, 2, half_b, left),
            SH_OWN: (0, 0, pl.ds(0, bw), partner),
            SH_LA: (3, 3, half_a, partner), SH_LB: (3, 3, half_b, partner),
            SH_RA: (1, 1, half_a, partner), SH_RB: (1, 1, half_b, partner),
            SH_OA: (2, 2, half_a, partner), SH_OB: (2, 2, half_b, partner),
        }[kind])

    def send_pair(h, d):
        pltpu.make_async_remote_copy(
            src_ref=pb.at[h, d, theirs, :], dst_ref=pr.at[h, d], send_sem=ssem.at[h, d, 0], recv_sem=rsem.at[h, d, 0],
            device_id={"tp": partner}, device_id_type=pl.DeviceIdType.MESH,
        ).start()

    def send(h, *kinds, p=None):
        for kind in kinds:
            msg(h, kind, p).start()

    def recv(h, *kinds, p=None):
        for kind in kinds:
            with scope("recv%d" % kind):
                msg(h, kind, p).wait_recv()

    def pair_sum(h, d, cols, p=None):
        return pb[h, d, mine_of(p), cols].astype(F32) + pr[h, d, piece(p), cols].astype(F32)

    def ev1(h):
        recv(h, PAIR + 2)
        for p in range(2):
            sb[h, 0, piece(p), :] = pair_sum(h, 2, half_a, p).astype(BF16)
            sb[h, 1, piece(p), :] = pair_sum(h, 2, half_b, p).astype(BF16)
            send(h, M1R, M1L, p=p)

    def ev2(h):
        recv(h, PAIR + 1)
        sb[h, 2] = pair_sum(h, 1, half_b).astype(BF16)
        recv(h, PAIR + 3)
        sb[h, 3] = pair_sum(h, 3, half_a).astype(BF16)
        send(h, M2R, M2L)

    def ev3(h):
        for p in range(2):
            recv(h, M1R, p=p)
            sb[h, 4, piece(p), :] = (pair_sum(h, 1, half_a, p) + rb[h, 0, piece(p), :].astype(F32)).astype(BF16)
            send(h, M3R, p=p)
            recv(h, M1L, p=p)
            sb[h, 5, piece(p), :] = (pair_sum(h, 3, half_b, p) + rb[h, 1, piece(p), :].astype(F32)).astype(BF16)
            send(h, M3L, p=p)

    def ev4(h):
        recv(h, PAIR + 0, M2L, M2R)

        def own_sum(cols, plain, summed, p):
            xg[h, 0, mine_of(p), cols] = (xg[h, 0, mine_of(p), cols].astype(F32) + (
                pair_sum(h, 0, cols, p) + rb[h, plain, piece(p), :].astype(F32)
                + rb[h, summed, piece(p), :].astype(F32))).astype(BF16)

        for p in range(2):
            recv(h, M3R, p=p)
            own_sum(half_a, 3, 4, p)
            send(h, OWN_RA, p=p)
            recv(h, M3L, p=p)
            own_sum(half_b, 2, 5, p)
            send(h, OWN_LB, p=p)
        send(h, OWN_LA, OWN_RB, SH_OWN)

    def ev5(h):
        for p in range(2):
            recv(h, OWN_RA, p=p)
            send(h, FWD_R, p=p)
            recv(h, OWN_LB, p=p)
            send(h, FWD_L, p=p)
        send(h, SH_LA, SH_RB)

    def ev6(h):
        recv(h, OWN_LA)
        send(h, SH_RA)
        recv(h, OWN_RB)
        send(h, SH_LB)

    def ev7(h):
        for p in range(2):
            recv(h, FWD_R, p=p)
            send(h, SH_OA, p=p)
            recv(h, FWD_L, p=p)
            send(h, SH_OB, p=p)

    def ev8(h):
        recv(h, SH_OWN, SH_LA, SH_LB, SH_RA, SH_RB)
        for p in range(2):
            recv(h, SH_OA, SH_OB, p=p)
        with scope("sent"):
            for kind in range(KINDS):
                for p in (0, 1) if kind in SPLIT else (None,):
                    msg(h, kind, p).wait_send()

    def normalise(l, h, which):
        tiles = bw // 128

        def x_tile(r, t):
            return xg[h, r, :, pl.ds(pl.multiple_of(t * 128, 128), 128)].astype(F32)

        def over_blocks(fn, init):
            def one(r, c):
                for t in range(tiles):
                    c = fn(r, t, c)
                return c
            return lax.fori_loop(0, num_chips, one, init)

        zero = jnp.zeros((rows, 128), F32)
        with scope("norm"):
            total = over_blocks(lambda r, t, c: c + x_tile(r, t), zero)
            mean = jnp.sum(total, axis=1, keepdims=True) * (1.0 / model_dim)

            def add_square(r, t, c):
                d = x_tile(r, t) - mean
                return c + d * d

            sq = jnp.sum(over_blocks(add_square, zero), axis=1, keepdims=True)
            rstd = lax.rsqrt(sq * (1.0 / model_dim) + 1e-5)

            def scaled(r, c):
                for t in range(tiles):
                    g = gains[which, l, r, :, t * 128:(t + 1) * 128]
                    a_buf[r, :, t * 128:(t + 1) * 128] = ((x_tile(r, t) - mean) * rstd * g).astype(BF16)
                return c

            lax.fori_loop(0, num_chips, scaled, 0)

    def dot_all(lhs, rhs):
        return sum(jnp.dot(a, b, preferred_element_type=F32) for a, b in zip(lhs, rhs))

    def attn_steps(l, h):
        my_rows = pl.ds(pl.multiple_of(h * rows, rows), rows)

        def ln():
            normalise(l, h, 0)

            @pl.when(l + h == 0)
            def _():
                load(0, "q", 4, 4)
                load(0, "q", 5, 5)
                load(0, "o", 0, 6)
                load(0, "o", 1, 7)

        def qkv_main():
            @pl.when(h == 0)
            def _():
                wait_w(0, 1, 2, 3)

            with scope("mm_qkv"):
                part = dot_all([a_buf[r] for r in range(4)], [w[r] for r in range(4)])
                for t in range(10):
                    qkv[t, my_rows, :] = part[:, t * head_dim:(t + 1) * head_dim].astype(BF16)

            @pl.when(h == 1)
            def _():
                for r in range(4):
                    load(l, "u", 4 + r, r)

            @pl.when(l + h == 0)
            def _():
                for r in range(4):
                    load(0, "u", r, 8 + r)

        def qkv_rest():
            @pl.when(h == 0)
            def _():
                wait_w(4, 5)

            with scope("mm_qkv2"):
                part = dot_all([a_buf[r] for r in range(4)],
                               [w[4 + r // 2, :, pl.ds((r % 2) * hw, hw)] for r in range(4)])
                for t in range(5):
                    qkv[10 + t, my_rows, :] = part[:, t * head_dim:(t + 1) * head_dim].astype(BF16)

            @pl.when(h == 1)
            def _():
                load(l, "d", 0, 4)
                load(l, "d", 1, 5)

        def attend_half(static_h):
            at = pl.ds(static_h * rows, rows)
            shape = (rows, 2 * rows)
            q_pos = static_h * rows + lax.broadcasted_iota(jnp.int32, shape, 0)
            keep = lax.broadcasted_iota(jnp.int32, shape, 1) <= q_pos
            scale = 1.0 / math.sqrt(head_dim)
            with scope("attn"):
                for n in range(heads):
                    s = lax.dot_general(qkv[3 * n, at, :], qkv[3 * n + 1], (((1,), (1,)), ((), ())),
                                        preferred_element_type=F32) * scale
                    s = jnp.where(keep, s, -1e30)
                    p = jnp.exp(s - jnp.max(s, axis=1, keepdims=True))
                    total = jnp.sum(p, axis=1, keepdims=True)
                    mix = jnp.dot(p.astype(BF16), qkv[3 * n + 2], preferred_element_type=F32)
                    o_buf[:, n * head_dim:(n + 1) * head_dim] = (mix / total).astype(BF16)

        def attend():
            for static_h in range(2):
                pl.when(h == static_h)(functools.partial(attend_half, static_h))

        def prod(n):
            d = ORDER[n]
            s = 6 + n // 2
            if n % 2 == 0:
                @pl.when(h == 0)
                def _():
                    wait_w(s)

            with scope("mm_out"):
                pb[h, d] = jnp.dot(o_buf[...], w[s, pl.ds((n % 2) * hw, hw), :],
                                   preferred_element_type=F32).astype(BF16)
            send(h, PAIR + d)
            if n % 2 == 1:
                @pl.when(h == 1)
                def _():
                    load(l, "d", 2 + n // 2, s)

        return [ln, qkv_main, qkv_rest, attend] + [functools.partial(prod, n) for n in range(4)]

    def mlp_steps(l, h):
        def ln():
            normalise(l, h, 1)

        def up(n):
            base = 8 + n * (4 * h - 8)

            @pl.when((h == 0) | (n == 1))
            def _():
                wait_w(*[base + r for r in range(4)])

            with scope("mm_up"):
                part = dot_all([a_buf[r] for r in range(4)], [w[base + r] for r in range(4)])
                h_buf[n] = jax.nn.gelu(part, approximate=True).astype(BF16)

            @pl.when(h == 1 - n)
            def _():
                for r in range(4):
                    load(l, "d", 4 + r, base + r)

            @pl.when(h * n == 1)
            def _():
                load_next(l, "q", 4, 4)
                load_next(l, "q", 5, 5)
                load_next(l, "o", 0, 6)
                load_next(l, "o", 1, 7)

        def prod(n):
            d = 2 + n + (n // 2) * (1 - 2 * n)
            s0 = lax.rem(4 + 2 * n, 8)
            s1 = 2 * n + 4 * (n // 2)
            s = s0 + h * (s1 - s0)
            wait_w(s, s + 1)
            with scope("mm_down"):
                part = dot_all([h_buf[0], h_buf[1]], [w[s], w[s + 1]])
                pb[h, d] = part.astype(BF16)
            send_pair(h, d)
            for k in range(4):
                for i in range(2):
                    @pl.when((n == k) & (h == 0))
                    def _():
                        if k < 2:
                            load(l, "u", 4 + 2 * k + i, s0 + i)
                        else:
                            load(l, "d", 2 * (k - 2) + i, s0 + i)

                    @pl.when((n == k) & (h == 1))
                    def _():
                        if k < 2:
                            load_next(l, "q", 2 * k + i, s1 + i)
                        else:
                            load_next(l, "u", 2 * (k - 2) + i, s1 + i)

        return ln, up, prod

    def run_attn(l, h, plan):
        for n, step in enumerate(attn_steps(l, h)):
            step()
            for whose, ev in plan.get(n, ()):
                if whose == SELF:
                    ev(h)
                else:
                    pl.when(l + h > 0)(functools.partial(ev, 1 - h))

    def run_mlp(l, h, plan):
        ln, up, prod = mlp_steps(l, h)

        def events(n, k, at):
            for whose, ev in plan.get(at, ()):
                pl.when(n == k)(functools.partial(ev, h if whose == SELF else 1 - h))

        def up_step(n, c):
            up(n)
            for k in range(2):
                events(n, k, 1 + k)
            return c

        def prod_step(n, c):
            prod(n)
            for k in range(3):
                events(n, k, 3 + k)
            return c

        ln()
        lax.fori_loop(0, 2, up_step, 0)
        lax.fori_loop(0, num_chips, prod_step, 0)
        for whose, ev in plan[6]:
            ev(h if whose == SELF else 1 - h)

    def x_copy(h, r):
        return pltpu.make_async_copy(x_hbm.at[pl.ds(h * rows, rows), block(r)], xg.at[h, r], xsem.at[h, r])

    def out_copy(h, r):
        return pltpu.make_async_copy(xg.at[h, r], out.at[pl.ds(h * rows, rows), block(r)], xsem.at[h, r])

    for h in range(2):
        for r in range(num_chips):
            x_copy(h, r).start()
    load(0, "q", 0, 0)
    barrier = pltpu.get_barrier_semaphore()
    for n in range(1, tp):
        pl.semaphore_signal(barrier, inc=1, device_id={"tp": lax.rem(me + n, tp)},
                            device_id_type=pl.DeviceIdType.MESH)
    qkv[...] = jnp.zeros_like(qkv)
    for k, gain in enumerate((g1, g2)):
        for l in range(num_layers):
            for r in range(num_chips):
                gains[k, l, r] = gain[pl.ds(l, 1), block(r)]
    with scope("xwait"):
        for h in range(2):
            for r in range(num_chips):
                x_copy(h, r).wait()
    for r in range(1, 4):
        load(0, "q", r, r)
    with scope("bar"):
        pl.semaphore_wait(barrier, tp - 1)

    def layer(l, c):
        def attn_half(h, c):
            run_attn(l, h, {
                1: [(OTHER, ev4)],
                5: [(OTHER, ev5)],
                6: [(SELF, ev1), (OTHER, ev6)],
                7: [(SELF, ev2), (OTHER, ev7), (SELF, ev3), (OTHER, ev8)],
            })
            return c

        def mlp_half(h, c):
            run_mlp(l, h, {
                1: [(OTHER, ev4)],
                3: [(OTHER, ev5)],
                4: [(SELF, ev1)],
                5: [(OTHER, ev6)],
                6: [(SELF, ev2), (OTHER, ev7), (SELF, ev3), (OTHER, ev8)],
            })
            return c

        lax.fori_loop(0, 2, attn_half, 0)
        lax.fori_loop(0, 2, mlp_half, 0)
        return c

    lax.fori_loop(0, num_layers, layer, 0)
    ev4(1)
    for r in range(num_chips):
        out_copy(0, r).start()
    for ev in (ev5, ev6, ev7, ev8):
        ev(1)
    for r in range(num_chips):
        out_copy(1, r).start()
    with scope("outw"):
        for h in range(2):
            for r in range(num_chips):
                out_copy(h, r).wait()


def solution(mesh):
    tp = mesh.shape["tp"]
    num_chips = tp // 2

    def device_fn(act_in, w_qkv, w_out, w_up, w_down, gain_one, gain_two):
        seq, model_dim = act_in.shape
        num_layers, _, heads, _, head_dim = w_qkv.shape
        ffn = w_up.shape[2]
        bw = model_dim // num_chips
        half, hw = seq // 2, bw // 2
        wq = jnp.transpose(w_qkv, (0, 2, 3, 1, 4)).reshape(num_layers, heads * 3, model_dim, head_dim)
        wo = w_out.reshape(num_layers, heads * head_dim, model_dim)
        vmem = pl.BlockSpec(memory_space=pltpu.VMEM)
        hbm = pl.BlockSpec(memory_space=pl.ANY)
        return pl.pallas_call(
            functools.partial(layer_kernel, num_layers, num_chips, heads, head_dim),
            out_shape=jax.ShapeDtypeStruct((seq, model_dim), BF16),
            in_specs=[hbm] * 5 + [vmem] * 2,
            out_specs=hbm,
            scratch_shapes=[
                pltpu.VMEM((2, num_chips, half, bw), BF16),
                pltpu.VMEM((num_chips, half, bw), BF16),
                pltpu.VMEM((2, num_chips, half, bw), BF16),
                pltpu.VMEM((2, num_chips, half // 2, bw), BF16),
                pltpu.VMEM((2, 6, half // 2, hw), BF16),
                pltpu.VMEM((2, 6, half // 2, hw), BF16),
                pltpu.VMEM((heads * 3, seq, head_dim), BF16),
                pltpu.VMEM((half, heads * head_dim), BF16),
                pltpu.VMEM((ffn // bw, half, bw), BF16),
                pltpu.VMEM((2, num_layers, num_chips, 1, bw), F32),
                pltpu.VMEM((SLOTS, bw, bw), BF16),
                pltpu.SemaphoreType.DMA((SLOTS,)),
                pltpu.SemaphoreType.DMA((2, num_chips)),
                pltpu.SemaphoreType.DMA((2, KINDS, 2)),
                pltpu.SemaphoreType.DMA((2, KINDS, 2)),
            ],
            compiler_params=pltpu.CompilerParams(
                collective_id=0, has_side_effects=True, vmem_limit_bytes=54 * 2 ** 20),
            name="layers",
        )(act_in, wq, wo, w_up, w_down, gain_one, gain_two)

    return jax.shard_map(
        device_fn,
        mesh=mesh,
        in_specs=(
            P("dp", None),
            P(None, None, "tp", None, None),
            P(None, "tp", None, None),
            P(None, None, "tp"),
            P(None, "tp", None),
            P(None, None),
            P(None, None),
        ),
        out_specs=P("dp", None),
        check_vma=False,
    )
```

```python
import functools
import math

import jax
import jax.numpy as jnp
from jax import lax
from jax.experimental import pallas as pl
from jax.experimental.pallas import tpu as pltpu
from jax.sharding import PartitionSpec as P

F32 = jnp.float32
BF16 = jnp.bfloat16
SLOTS = 12
PAIR, M1R, M1L, M2R, M2L, M3R, M3L = 0, 4, 5, 6, 7, 8, 9
OWN_RA, OWN_RB, OWN_LA, OWN_LB, FWD_R, FWD_L = 10, 11, 12, 13, 14, 15
SH_OWN, SH_LA, SH_LB, SH_RA, SH_RB, SH_OA, SH_OB = 16, 17, 18, 19, 20, 21, 22
KINDS = 23
ORDER = (2, 3, 1, 0)
SPLIT = (M1R, M1L, M3R, M3L, OWN_RA, OWN_LB, FWD_R, FWD_L, SH_OA, SH_OB)
SELF, OTHER = 0, 1


def layer_kernel(
    num_layers, num_chips, heads, head_dim,
    x_hbm, wq, wo, w1, w2, g1, g2, out,
    xg, a_buf, pb, pr, sb, rb, qkv, o_buf, h_buf, gains, st, w,
    wsem, xsem, ssem, rsem,
):
    rows = xg.shape[2]
    bw = xg.shape[3]
    own = rows // 2
    hw = bw // 2
    model_dim = num_chips * bw
    tp = 2 * num_chips
    me = lax.axis_index("tp")
    chip = me // 2
    core = me % 2
    mine = pl.ds(pl.multiple_of(core * own, own), own)
    theirs = pl.ds(pl.multiple_of((1 - core) * own, own), own)
    scope = jax.named_scope

    def chip_at(r):
        return lax.rem(chip + r, num_chips)

    def block(r):
        return pl.ds(pl.multiple_of(chip_at(r) * bw, bw), bw)

    right = chip_at(1) * 2 + core
    left = chip_at(3) * 2 + core
    partner = chip * 2 + (1 - core)
    half_a = pl.ds(0, hw)
    half_b = pl.ds(hw, hw)

    def load(l, what, n, s):
        res = []

        def slab(t, r, col):
            res.append((wq.at[l, t, block(r), :], w.at[s, :, pl.ds(col, head_dim)]))

        if what == "q" and n < 4:
            for t in range(10):
                slab(t, n, t * head_dim)
        elif what == "q":
            for i in range(2):
                for t in range(5):
                    slab(10 + t, 2 * (n - 4) + i, i * hw + t * head_dim)
        elif what == "o":
            for i in range(2):
                res.append((wo.at[l, :, block(ORDER[2 * n + i])], w.at[s, pl.ds(i * hw, hw), :]))
        elif what == "u":
            res.append((w1.at[l, block(n % 4), pl.ds((n // 4) * bw, bw)], w.at[s]))
        else:
            res.append((w2.at[l, pl.ds((n % 2) * bw, bw), block(ORDER[n // 2])], w.at[s]))
        for a, b in res:
            pltpu.make_async_copy(a, b, wsem.at[s]).start()

    def load_next(l, what, n, s):
        @pl.when(l + 1 < num_layers)
        def _():
            load(l + 1, what, n, s)

    def wait_w(*slots):
        with scope("wwait"):
            for s in slots:
                pltpu.make_async_copy(w.at[s], w.at[s], wsem.at[s]).wait()

    part = own // 2

    def piece(p):
        return pl.ds(0, own) if p is None else pl.ds(p * part, part)

    def mine_of(p):
        return mine if p is None else pl.ds(pl.multiple_of(core * own + p * part, part), part)

    def msg(h, kind, p=None):
        n = 0 if p is None else p

        def rc(src, dst, dev):
            return pltpu.make_async_remote_copy(
                src_ref=src, dst_ref=dst, send_sem=ssem.at[h, kind, n], recv_sem=rsem.at[h, kind, n],
                device_id={"tp": dev}, device_id_type=pl.DeviceIdType.MESH,
            )

        def move(r_from, r_to, cols, dev):
            return rc(xg.at[h, r_from, mine_of(p), cols], xg.at[h, r_to, mine_of(p), cols], dev)

        if kind < 4:
            return rc(pb.at[h, kind, theirs, :], pr.at[h, kind], partner)
        if kind <= M3L:
            k = kind - M1R
            return rc(sb.at[h, k, piece(p), :], rb.at[h, k, piece(p), :], right if k % 2 == 0 else left)
        return move(*{
            OWN_RA: (0, 3, half_a, right), OWN_RB: (0, 3, half_b, right),
            OWN_LA: (0, 1, half_a, left), OWN_LB: (0, 1, half_b, left),
            FWD_R: (3, 2, half_a, right), FWD_L: (1, 2, half_b, left),
            SH_OWN: (0, 0, pl.ds(0, bw), partner),
            SH_LA: (3, 3, half_a, partner), SH_LB: (3, 3, half_b, partner),
            SH_RA: (1, 1, half_a, partner), SH_RB: (1, 1, half_b, partner),
            SH_OA: (2, 2, half_a, partner), SH_OB: (2, 2, half_b, partner),
        }[kind])

    def send_pair(h, d):
        pltpu.make_async_remote_copy(
            src_ref=pb.at[h, d, theirs, :], dst_ref=pr.at[h, d], send_sem=ssem.at[h, d, 0], recv_sem=rsem.at[h, d, 0],
            device_id={"tp": partner}, device_id_type=pl.DeviceIdType.MESH,
        ).start()

    def send(h, *kinds, p=None):
        for kind in kinds:
            msg(h, kind, p).start()

    def recv(h, *kinds, p=None):
        for kind in kinds:
            with scope("recv%d" % kind):
                msg(h, kind, p).wait_recv()

    def pair_sum(h, d, cols, p=None):
        return pb[h, d, mine_of(p), cols].astype(F32) + pr[h, d, piece(p), cols].astype(F32)

    def ev1(h):
        recv(h, PAIR + 2)
        for p in range(2):
            sb[h, 0, piece(p), :] = pair_sum(h, 2, half_a, p).astype(BF16)
            sb[h, 1, piece(p), :] = pair_sum(h, 2, half_b, p).astype(BF16)
            send(h, M1R, M1L, p=p)

    def ev2(h):
        recv(h, PAIR + 1)
        sb[h, 2] = pair_sum(h, 1, half_b).astype(BF16)
        recv(h, PAIR + 3)
        sb[h, 3] = pair_sum(h, 3, half_a).astype(BF16)
        send(h, M2R, M2L)

    def ev3(h):
        for p in range(2):
            recv(h, M1R, p=p)
            sb[h, 4, piece(p), :] = (pair_sum(h, 1, half_a, p) + rb[h, 0, piece(p), :].astype(F32)).astype(BF16)
            send(h, M3R, p=p)
            recv(h, M1L, p=p)
            sb[h, 5, piece(p), :] = (pair_sum(h, 3, half_b, p) + rb[h, 1, piece(p), :].astype(F32)).astype(BF16)
            send(h, M3L, p=p)

    def ev4(h):
        recv(h, PAIR + 0, M2L, M2R)

        def own_sum(cols, plain, summed, p):
            xg[h, 0, mine_of(p), cols] = (xg[h, 0, mine_of(p), cols].astype(F32) + (
                pair_sum(h, 0, cols, p) + rb[h, plain, piece(p), :].astype(F32)
                + rb[h, summed, piece(p), :].astype(F32))).astype(BF16)

        for p in range(2):
            recv(h, M3R, p=p)
            own_sum(half_a, 3, 4, p)
            send(h, OWN_RA, p=p)
            recv(h, M3L, p=p)
            own_sum(half_b, 2, 5, p)
            send(h, OWN_LB, p=p)
        send(h, OWN_LA, OWN_RB, SH_OWN)

    def ev5(h):
        for p in range(2):
            recv(h, OWN_RA, p=p)
            send(h, FWD_R, p=p)
            recv(h, OWN_LB, p=p)
            send(h, FWD_L, p=p)
        send(h, SH_LA, SH_RB)

    def ev6(h):
        recv(h, OWN_LA)
        send(h, SH_RA)
        recv(h, OWN_RB)
        send(h, SH_LB)

    def ev7(h):
        for p in range(2):
            recv(h, FWD_R, p=p)
            send(h, SH_OA, p=p)
            recv(h, FWD_L, p=p)
            send(h, SH_OB, p=p)

    def ev_near(h):
        recv(h, SH_OWN, SH_LA, SH_LB, SH_RA, SH_RB)

    def ev_near_stats(h):
        ev_near(h)
        near_stats(h)

    def ev8(h):
        for p in range(2):
            recv(h, SH_OA, SH_OB, p=p)
        with scope("sent"):
            for kind in range(KINDS):
                for p in (0, 1) if kind in SPLIT else (None,):
                    msg(h, kind, p).wait_send()

    def x_copy(h, r):
        src = x_hbm.at[pl.ds(pl.multiple_of(h * rows, rows), rows), block(r)]
        return pltpu.make_async_copy(src, xg.at[h, r], xsem.at[h, r])

    tiles = bw // 128

    def x_tile(h, r, t):
        return xg[h, r, :, t * 128:(t + 1) * 128].astype(F32)

    def block_stats(h, r):
        total = x_tile(h, r, 0)
        for t in range(1, tiles):
            total = total + x_tile(h, r, t)
        mean = jnp.sum(total, axis=1, keepdims=True) * (1.0 / bw)
        sq = jnp.zeros((rows, 128), F32)
        for t in range(tiles):
            d = x_tile(h, r, t) - mean
            sq = sq + d * d
        m2 = jnp.sum(sq, axis=1, keepdims=True)
        st[r, 0] = jnp.broadcast_to(mean, (rows, 128))
        st[r, 1] = jnp.broadcast_to(m2, (rows, 128))

    def near_stats(h):
        def one(n, c):
            block_stats(h, n + n // 2)
            return c

        with scope("stats"):
            lax.fori_loop(0, num_chips - 1, one, 0)

    def normalise(l, h, which):
        with scope("norm"):
            block_stats(h, 2)
            mean = (st[0, 0] + st[1, 0] + st[2, 0] + st[3, 0]) * (1.0 / num_chips)
            m2 = st[0, 1] + st[1, 1] + st[2, 1] + st[3, 1]
            for r in range(num_chips):
                d = st[r, 0] - mean
                m2 = m2 + bw * (d * d)
            rstd = lax.rsqrt(m2 * (1.0 / model_dim) + 1e-5)

            def scaled(r, c):
                for t in range(tiles):
                    g = gains[which, l, r, :, t * 128:(t + 1) * 128]
                    a_buf[r, :, t * 128:(t + 1) * 128] = ((x_tile(h, r, t) - mean) * rstd * g).astype(BF16)
                return c

            lax.fori_loop(0, num_chips, scaled, 0)

    def dot_all(lhs, rhs):
        return sum(jnp.dot(a, b, preferred_element_type=F32) for a, b in zip(lhs, rhs))

    def attn_steps(l, h):
        my_rows = pl.ds(pl.multiple_of(h * rows, rows), rows)

        def ln():
            @pl.when(l == 0)
            def _():
                for r in range(num_chips):
                    x_copy(h, r).wait()
                near_stats(h)

            normalise(l, h, 0)

            @pl.when(l + h == 0)
            def _():
                load(0, "q", 4, 4)
                load(0, "q", 5, 5)
                load(0, "o", 0, 6)
                load(0, "o", 1, 7)

        def qkv_main():
            @pl.when(h == 0)
            def _():
                wait_w(0, 1, 2, 3)

            with scope("mm_qkv"):
                part = dot_all([a_buf[r] for r in range(4)], [w[r] for r in range(4)])
                for t in range(10):
                    qkv[t, my_rows, :] = part[:, t * head_dim:(t + 1) * head_dim].astype(BF16)

            @pl.when(h == 1)
            def _():
                for r in range(4):
                    load(l, "u", 4 + r, r)

            @pl.when(l + h == 0)
            def _():
                for r in range(4):
                    load(0, "u", r, 8 + r)

        def qkv_rest():
            @pl.when(h == 0)
            def _():
                wait_w(4, 5)

            with scope("mm_qkv2"):
                part = dot_all([a_buf[r] for r in range(4)],
                               [w[4 + r // 2, :, pl.ds((r % 2) * hw, hw)] for r in range(4)])
                for t in range(5):
                    qkv[10 + t, my_rows, :] = part[:, t * head_dim:(t + 1) * head_dim].astype(BF16)

            @pl.when(h == 1)
            def _():
                load(l, "d", 0, 4)
                load(l, "d", 1, 5)

        def attend_half(static_h):
            at = pl.ds(static_h * rows, rows)
            shape = (rows, 2 * rows)
            q_pos = static_h * rows + lax.broadcasted_iota(jnp.int32, shape, 0)
            keep = lax.broadcasted_iota(jnp.int32, shape, 1) <= q_pos
            scale = 1.0 / math.sqrt(head_dim)
            with scope("attn"):
                for n in range(heads):
                    s = lax.dot_general(qkv[3 * n, at, :], qkv[3 * n + 1], (((1,), (1,)), ((), ())),
                                        preferred_element_type=F32) * scale
                    s = jnp.where(keep, s, -1e30)
                    p = jnp.exp(s - jnp.max(s, axis=1, keepdims=True))
                    total = jnp.sum(p, axis=1, keepdims=True)
                    mix = jnp.dot(p.astype(BF16), qkv[3 * n + 2], preferred_element_type=F32)
                    o_buf[:, n * head_dim:(n + 1) * head_dim] = (mix / total).astype(BF16)

        def attend():
            for static_h in range(2):
                pl.when(h == static_h)(functools.partial(attend_half, static_h))

        def prod(n):
            d = ORDER[n]
            s = 6 + n // 2
            if n % 2 == 0:
                @pl.when(h == 0)
                def _():
                    wait_w(s)

            with scope("mm_out"):
                pb[h, d] = jnp.dot(o_buf[...], w[s, pl.ds((n % 2) * hw, hw), :],
                                   preferred_element_type=F32).astype(BF16)
            send(h, PAIR + d)
            if n % 2 == 1:
                @pl.when(h == 1)
                def _():
                    load(l, "d", 2 + n // 2, s)

        return [ln, qkv_main, qkv_rest, attend] + [functools.partial(prod, n) for n in range(4)]

    def mlp_steps(l, h):
        def ln():
            normalise(l, h, 1)

        def up(n):
            base = 8 + n * (4 * h - 8)

            @pl.when((h == 0) | (n == 1))
            def _():
                wait_w(*[base + r for r in range(4)])

            with scope("mm_up"):
                part = dot_all([a_buf[r] for r in range(4)], [w[base + r] for r in range(4)])
                h_buf[n] = jax.nn.gelu(part, approximate=True).astype(BF16)

            @pl.when(h == 1 - n)
            def _():
                for r in range(4):
                    load(l, "d", 4 + r, base + r)

            @pl.when(h * n == 1)
            def _():
                load_next(l, "q", 4, 4)
                load_next(l, "q", 5, 5)
                load_next(l, "o", 0, 6)
                load_next(l, "o", 1, 7)

        def prod(n):
            d = 2 + n + (n // 2) * (1 - 2 * n)
            s0 = lax.rem(4 + 2 * n, 8)
            s1 = 2 * n + 4 * (n // 2)
            s = s0 + h * (s1 - s0)
            wait_w(s, s + 1)
            with scope("mm_down"):
                part = dot_all([h_buf[0], h_buf[1]], [w[s], w[s + 1]])
                pb[h, d] = part.astype(BF16)
            send_pair(h, d)
            for k in range(4):
                for i in range(2):
                    @pl.when((n == k) & (h == 0))
                    def _():
                        if k < 2:
                            load(l, "u", 4 + 2 * k + i, s0 + i)
                        else:
                            load(l, "d", 2 * (k - 2) + i, s0 + i)

                    @pl.when((n == k) & (h == 1))
                    def _():
                        if k < 2:
                            load_next(l, "q", 2 * k + i, s1 + i)
                        else:
                            load_next(l, "u", 2 * (k - 2) + i, s1 + i)

        return ln, up, prod

    def run_attn(l, h, plan):
        for n, step in enumerate(attn_steps(l, h)):
            step()
            for whose, ev in plan.get(n, ()):
                if whose == SELF:
                    ev(h)
                else:
                    pl.when(l + h > 0)(functools.partial(ev, 1 - h))

    def run_mlp(l, h, plan):
        ln, up, prod = mlp_steps(l, h)

        def events(n, k, at):
            for whose, ev in plan.get(at, ()):
                pl.when(n == k)(functools.partial(ev, h if whose == SELF else 1 - h))

        def up_step(n, c):
            up(n)
            for k in range(2):
                events(n, k, 1 + k)
            return c

        def prod_step(n, c):
            prod(n)
            for k in range(3):
                events(n, k, 3 + k)
            return c

        ln()
        lax.fori_loop(0, 2, up_step, 0)
        lax.fori_loop(0, num_chips, prod_step, 0)
        for whose, ev in plan[6]:
            ev(h if whose == SELF else 1 - h)

    def put_out(h):
        with scope("put"):
            for r in range(num_chips):
                out[pl.ds(h * rows, rows), block(r)] = xg[h, r]

    for r in range(num_chips):
        x_copy(0, r).start()
    load(0, "q", 0, 0)
    load(0, "q", 1, 1)
    barrier = pltpu.get_barrier_semaphore()
    for n in range(1, tp):
        pl.semaphore_signal(barrier, inc=1, device_id={"tp": lax.rem(me + n, tp)},
                            device_id_type=pl.DeviceIdType.MESH)
    qkv[...] = jnp.zeros_like(qkv)
    for k, gain in enumerate((g1, g2)):
        for l in range(num_layers):
            for r in range(num_chips):
                gains[k, l, r] = gain[pl.ds(l, 1), block(r)]
    for r in range(num_chips):
        x_copy(1, r).start()
    for r in range(2, 4):
        load(0, "q", r, r)
    with scope("bar"):
        pl.semaphore_wait(barrier, tp - 1)

    def layer(l, c):
        def attn_half(h, c):
            run_attn(l, h, {
                1: [(OTHER, ev4)],
                5: [(OTHER, ev5)],
                6: [(SELF, ev1), (OTHER, ev6)],
                7: [(SELF, ev2), (OTHER, ev_near_stats), (OTHER, ev7), (SELF, ev3), (OTHER, ev8)],
            })
            return c

        def mlp_half(h, c):
            run_mlp(l, h, {
                1: [(OTHER, ev4)],
                3: [(OTHER, ev5)],
                4: [(SELF, ev1)],
                5: [(OTHER, ev6)],
                6: [(SELF, ev2), (OTHER, ev_near_stats), (OTHER, ev7), (SELF, ev3), (OTHER, ev8)],
            })
            return c

        lax.fori_loop(0, 2, attn_half, 0)
        lax.fori_loop(0, 2, mlp_half, 0)
        return c

    lax.fori_loop(0, num_layers, layer, 0)
    ev4(1)
    put_out(0)
    for ev in (ev5, ev6, ev_near, ev7, ev8):
        ev(1)
    put_out(1)


def solution(mesh):
    tp = mesh.shape["tp"]
    num_chips = tp // 2

    def device_fn(act_in, w_qkv, w_out, w_up, w_down, gain_one, gain_two):
        seq, model_dim = act_in.shape
        num_layers, _, heads, _, head_dim = w_qkv.shape
        ffn = w_up.shape[2]
        bw = model_dim // num_chips
        half, hw = seq // 2, bw // 2
        wq = jnp.transpose(w_qkv, (0, 2, 3, 1, 4)).reshape(num_layers, heads * 3, model_dim, head_dim)
        wo = w_out.reshape(num_layers, heads * head_dim, model_dim)
        vmem = pl.BlockSpec(memory_space=pltpu.VMEM)
        hbm = pl.BlockSpec(memory_space=pl.ANY)
        return pl.pallas_call(
            functools.partial(layer_kernel, num_layers, num_chips, heads, head_dim),
            out_shape=pltpu.VMEM((seq, model_dim), BF16),
            in_specs=[hbm] * 5 + [vmem] * 2,
            out_specs=vmem,
            scratch_shapes=[
                pltpu.VMEM((2, num_chips, half, bw), BF16),
                pltpu.VMEM((num_chips, half, bw), BF16),
                pltpu.VMEM((2, num_chips, half, bw), BF16),
                pltpu.VMEM((2, num_chips, half // 2, bw), BF16),
                pltpu.VMEM((2, 6, half // 2, hw), BF16),
                pltpu.VMEM((2, 6, half // 2, hw), BF16),
                pltpu.VMEM((heads * 3, seq, head_dim), BF16),
                pltpu.VMEM((half, heads * head_dim), BF16),
                pltpu.VMEM((ffn // bw, half, bw), BF16),
                pltpu.VMEM((2, num_layers, num_chips, 1, bw), F32),
                pltpu.VMEM((num_chips, 2, half, 128), F32),
                pltpu.VMEM((SLOTS, bw, bw), BF16),
                pltpu.SemaphoreType.DMA((SLOTS,)),
                pltpu.SemaphoreType.DMA((2, num_chips)),
                pltpu.SemaphoreType.DMA((2, KINDS, 2)),
                pltpu.SemaphoreType.DMA((2, KINDS, 2)),
            ],
            compiler_params=pltpu.CompilerParams(
                collective_id=0, has_side_effects=True, vmem_limit_bytes=54 * 2 ** 20),
            name="layers",
        )(act_in, wq, wo, w_up, w_down, gain_one, gain_two)

    return jax.shard_map(
        device_fn,
        mesh=mesh,
        in_specs=(
            P("dp", None),
            P(None, None, "tp", None, None),
            P(None, "tp", None, None),
            P(None, None, "tp"),
            P(None, "tp", None),
            P(None, None),
            P(None, None),
        ),
        out_specs=P("dp", None),
        check_vma=False,
    )
```

```python
import functools
import math

import jax
import jax.numpy as jnp
from jax import lax
from jax.experimental import pallas as pl
from jax.experimental.pallas import tpu as pltpu
from jax.sharding import PartitionSpec as P

F32 = jnp.float32
BF16 = jnp.bfloat16
SLOTS = 14
Q_SLOTS = (12, 13, 2, 3)
PAIR, M1R, M1L, M2R, M2L, M3R, M3L = 0, 4, 5, 6, 7, 8, 9
OWN_RA, OWN_RB, OWN_LA, OWN_LB, FWD_R, FWD_L = 10, 11, 12, 13, 14, 15
SH_OWN, SH_LA, SH_LB, SH_RA, SH_RB, SH_OA, SH_OB = 16, 17, 18, 19, 20, 21, 22
KINDS = 23
ORDER = (2, 3, 1, 0)
SPLIT = (M1R, M1L, M3R, M3L, OWN_RA, OWN_LB, FWD_R, FWD_L, SH_OA, SH_OB)
SELF, OTHER = 0, 1


def layer_kernel(
    num_layers, num_chips, heads, head_dim,
    x_hbm, wq, wo, w1, w2, g1, g2, out,
    xg, a_buf, pb, pr, sb, rb, qkv, o_buf, h_buf, gains, st, w,
    wsem, xsem, ssem, rsem,
):
    rows = xg.shape[2]
    bw = xg.shape[3]
    own = rows // 2
    hw = bw // 2
    model_dim = num_chips * bw
    tp = 2 * num_chips
    me = lax.axis_index("tp")
    chip = me // 2
    core = me % 2
    mine = pl.ds(pl.multiple_of(core * own, own), own)
    theirs = pl.ds(pl.multiple_of((1 - core) * own, own), own)
    scope = jax.named_scope

    def chip_at(r):
        return lax.rem(chip + r, num_chips)

    def block(r):
        return pl.ds(pl.multiple_of(chip_at(r) * bw, bw), bw)

    right = chip_at(1) * 2 + core
    left = chip_at(3) * 2 + core
    partner = chip * 2 + (1 - core)
    half_a = pl.ds(0, hw)
    half_b = pl.ds(hw, hw)

    def load(l, what, n, s):
        res = []

        def slab(t, r, col):
            res.append((wq.at[l, t, block(r), :], w.at[s, :, pl.ds(col, head_dim)]))

        if what == "q" and n < 4:
            for t in range(10):
                slab(t, n, t * head_dim)
        elif what == "q":
            for i in range(2):
                for t in range(5):
                    slab(10 + t, 2 * (n - 4) + i, i * hw + t * head_dim)
        elif what == "o":
            for i in range(2):
                res.append((wo.at[l, :, block(ORDER[2 * n + i])], w.at[s, pl.ds(i * hw, hw), :]))
        elif what == "u":
            res.append((w1.at[l, block(n % 4), pl.ds((n // 4) * bw, bw)], w.at[s]))
        else:
            res.append((w2.at[l, pl.ds((n % 2) * bw, bw), block(ORDER[n // 2])], w.at[s]))
        for a, b in res:
            pltpu.make_async_copy(a, b, wsem.at[s]).start()

    def load_next(l, what, n, s):
        @pl.when(l + 1 < num_layers)
        def _():
            load(l + 1, what, n, s)

    def wait_w(*slots):
        with scope("wwait"):
            for s in slots:
                pltpu.make_async_copy(w.at[s], w.at[s], wsem.at[s]).wait()

    part = own // 2

    def piece(p):
        return pl.ds(0, own) if p is None else pl.ds(p * part, part)

    def mine_of(p):
        return mine if p is None else pl.ds(pl.multiple_of(core * own + p * part, part), part)

    def msg(h, kind, p=None):
        n = 0 if p is None else p

        def rc(src, dst, dev):
            return pltpu.make_async_remote_copy(
                src_ref=src, dst_ref=dst, send_sem=ssem.at[h, kind, n], recv_sem=rsem.at[h, kind, n],
                device_id={"tp": dev}, device_id_type=pl.DeviceIdType.MESH,
            )

        def move(r_from, r_to, cols, dev):
            return rc(xg.at[h, r_from, mine_of(p), cols], xg.at[h, r_to, mine_of(p), cols], dev)

        if kind < 4:
            return rc(pb.at[h, kind, theirs, :], pr.at[h, kind], partner)
        if kind <= M3L:
            k = kind - M1R
            return rc(sb.at[h, k, piece(p), :], rb.at[h, k, piece(p), :], right if k % 2 == 0 else left)
        return move(*{
            OWN_RA: (0, 3, half_a, right), OWN_RB: (0, 3, half_b, right),
            OWN_LA: (0, 1, half_a, left), OWN_LB: (0, 1, half_b, left),
            FWD_R: (3, 2, half_a, right), FWD_L: (1, 2, half_b, left),
            SH_OWN: (0, 0, pl.ds(0, bw), partner),
            SH_LA: (3, 3, half_a, partner), SH_LB: (3, 3, half_b, partner),
            SH_RA: (1, 1, half_a, partner), SH_RB: (1, 1, half_b, partner),
            SH_OA: (2, 2, half_a, partner), SH_OB: (2, 2, half_b, partner),
        }[kind])

    def send_pair(h, d):
        pltpu.make_async_remote_copy(
            src_ref=pb.at[h, d, theirs, :], dst_ref=pr.at[h, d], send_sem=ssem.at[h, d, 0], recv_sem=rsem.at[h, d, 0],
            device_id={"tp": partner}, device_id_type=pl.DeviceIdType.MESH,
        ).start()

    def send(h, *kinds, p=None):
        for kind in kinds:
            msg(h, kind, p).start()

    def recv(h, *kinds, p=None):
        for kind in kinds:
            with scope("recv%d" % kind):
                msg(h, kind, p).wait_recv()

    def pair_sum(h, d, cols, p=None):
        return pb[h, d, mine_of(p), cols].astype(F32) + pr[h, d, piece(p), cols].astype(F32)

    def ev1(h):
        recv(h, PAIR + 2)
        for p in range(2):
            sb[h, 0, piece(p), :] = pair_sum(h, 2, half_a, p).astype(BF16)
            sb[h, 1, piece(p), :] = pair_sum(h, 2, half_b, p).astype(BF16)
            send(h, M1R, M1L, p=p)

    def ev2_left(h):
        recv(h, PAIR + 3)
        sb[h, 3] = pair_sum(h, 3, half_a).astype(BF16)
        send(h, M2L)

    def ev2_right(h):
        recv(h, PAIR + 1)
        sb[h, 2] = pair_sum(h, 1, half_b).astype(BF16)
        send(h, M2R)

    def ev3(h):
        for p in range(2):
            recv(h, M1R, p=p)
            sb[h, 4, piece(p), :] = (pair_sum(h, 1, half_a, p) + rb[h, 0, piece(p), :].astype(F32)).astype(BF16)
            send(h, M3R, p=p)
            recv(h, M1L, p=p)
            sb[h, 5, piece(p), :] = (pair_sum(h, 3, half_b, p) + rb[h, 1, piece(p), :].astype(F32)).astype(BF16)
            send(h, M3L, p=p)

    def ev4(h):
        recv(h, PAIR + 0, M2L, M2R)

        def own_sum(cols, plain, summed, p):
            xg[h, 0, mine_of(p), cols] = (xg[h, 0, mine_of(p), cols].astype(F32) + (
                pair_sum(h, 0, cols, p) + rb[h, plain, piece(p), :].astype(F32)
                + rb[h, summed, piece(p), :].astype(F32))).astype(BF16)

        for p in range(2):
            recv(h, M3R, p=p)
            own_sum(half_a, 3, 4, p)
            send(h, OWN_RA, p=p)
            recv(h, M3L, p=p)
            own_sum(half_b, 2, 5, p)
            send(h, OWN_LB, p=p)
        send(h, OWN_LA, OWN_RB, SH_OWN)

    def ev5(h):
        for p in range(2):
            recv(h, OWN_RA, p=p)
            send(h, FWD_R, p=p)
            recv(h, OWN_LB, p=p)
            send(h, FWD_L, p=p)
        send(h, SH_LA, SH_RB)

    def ev6(h):
        recv(h, OWN_LA)
        send(h, SH_RA)
        recv(h, OWN_RB)
        send(h, SH_LB)

    def ev7(h):
        for p in range(2):
            recv(h, FWD_R, p=p)
            send(h, SH_OA, p=p)
            recv(h, FWD_L, p=p)
            send(h, SH_OB, p=p)

    def ev_near(h):
        recv(h, SH_OWN, SH_LA, SH_LB, SH_RA, SH_RB)

    def ev_near_stats(h):
        ev_near(h)
        near_stats(h)

    def ev8(h):
        for p in range(2):
            recv(h, SH_OA, SH_OB, p=p)
        with scope("sent"):
            for kind in range(KINDS):
                for p in (0, 1) if kind in SPLIT else (None,):
                    msg(h, kind, p).wait_send()

    def x_copy(h, r):
        src = x_hbm.at[pl.ds(pl.multiple_of(h * rows, rows), rows), block(r)]
        return pltpu.make_async_copy(src, xg.at[h, r], xsem.at[h, r])

    tiles = bw // 128

    def x_tile(h, r, t):
        return xg[h, r, :, t * 128:(t + 1) * 128].astype(F32)

    def block_stats(h, r):
        total = x_tile(h, r, 0)
        for t in range(1, tiles):
            total = total + x_tile(h, r, t)
        mean = jnp.sum(total, axis=1, keepdims=True) * (1.0 / bw)
        sq = jnp.zeros((rows, 128), F32)
        for t in range(tiles):
            d = x_tile(h, r, t) - mean
            sq = sq + d * d
        m2 = jnp.sum(sq, axis=1, keepdims=True)
        st[r, 0] = jnp.broadcast_to(mean, (rows, 128))
        st[r, 1] = jnp.broadcast_to(m2, (rows, 128))

    def near_stats(h):
        def one(n, c):
            block_stats(h, n + n // 2)
            return c

        with scope("stats"):
            lax.fori_loop(0, num_chips - 1, one, 0)

    def normalise(l, h, which):
        with scope("norm"):
            block_stats(h, 2)
            mean = (st[0, 0] + st[1, 0] + st[2, 0] + st[3, 0]) * (1.0 / num_chips)
            m2 = st[0, 1] + st[1, 1] + st[2, 1] + st[3, 1]
            for r in range(num_chips):
                d = st[r, 0] - mean
                m2 = m2 + bw * (d * d)
            rstd = lax.rsqrt(m2 * (1.0 / model_dim) + 1e-5)

            def scaled(r, c):
                for t in range(tiles):
                    g = gains[which, l, r, :, t * 128:(t + 1) * 128]
                    a_buf[r, :, t * 128:(t + 1) * 128] = ((x_tile(h, r, t) - mean) * rstd * g).astype(BF16)
                return c

            lax.fori_loop(0, num_chips, scaled, 0)

    def dot_all(lhs, rhs):
        return sum(jnp.dot(a, b, preferred_element_type=F32) for a, b in zip(lhs, rhs))

    def attn_steps(l, h):
        my_rows = pl.ds(pl.multiple_of(h * rows, rows), rows)

        def ln():
            @pl.when(l == 0)
            def _():
                for r in range(num_chips):
                    x_copy(h, r).wait()
                near_stats(h)

            normalise(l, h, 0)

            @pl.when(l + h == 0)
            def _():
                load(0, "q", 4, 4)
                load(0, "q", 5, 5)
                load(0, "o", 0, 6)
                load(0, "o", 1, 7)

        def qkv_main():
            @pl.when(h == 0)
            def _():
                wait_w(*Q_SLOTS)

            with scope("mm_qkv"):
                for first, count in ((0, 4), (4, 4), (8, 2)):
                    part = dot_all([a_buf[r] for r in range(4)],
                                   [w[s, :, pl.ds(first * head_dim, count * head_dim)] for s in Q_SLOTS])
                    for t in range(count):
                        qkv[first + t, my_rows, :] = part[:, t * head_dim:(t + 1) * head_dim].astype(BF16)

            @pl.when(h == 1)
            def _():
                for r in range(4):
                    load(l, "u", 4 + r, r)
                load_next(l, "q", 0, Q_SLOTS[0])
                load_next(l, "q", 1, Q_SLOTS[1])

            @pl.when(l + h == 0)
            def _():
                for r in range(4):
                    load(0, "u", r, 8 + r)

        def qkv_rest():
            @pl.when(h == 0)
            def _():
                wait_w(4, 5)

            with scope("mm_qkv2"):
                for first, count in ((0, 4), (4, 1)):
                    part = dot_all([a_buf[r] for r in range(4)],
                                   [w[4 + r // 2, :, pl.ds((r % 2) * hw + first * head_dim, count * head_dim)]
                                    for r in range(4)])
                    for t in range(count):
                        qkv[10 + first + t, my_rows, :] = part[:, t * head_dim:(t + 1) * head_dim].astype(BF16)

            @pl.when(h == 1)
            def _():
                load(l, "d", 0, 4)
                load(l, "d", 1, 5)

        def attend_half(static_h):
            at = pl.ds(static_h * rows, rows)
            shape = (rows, 2 * rows)
            q_pos = static_h * rows + lax.broadcasted_iota(jnp.int32, shape, 0)
            keep = lax.broadcasted_iota(jnp.int32, shape, 1) <= q_pos
            scale = 1.0 / math.sqrt(head_dim)
            with scope("attn"):
                for n in range(heads):
                    s = lax.dot_general(qkv[3 * n, at, :], qkv[3 * n + 1], (((1,), (1,)), ((), ())),
                                        preferred_element_type=F32) * scale
                    s = jnp.where(keep, s, -1e30)
                    p = jnp.exp(s - jnp.max(s, axis=1, keepdims=True))
                    total = jnp.sum(p, axis=1, keepdims=True)
                    mix = jnp.dot(p.astype(BF16), qkv[3 * n + 2], preferred_element_type=F32)
                    o_buf[:, n * head_dim:(n + 1) * head_dim] = (mix / total).astype(BF16)

        def attend():
            for static_h in range(2):
                pl.when(h == static_h)(functools.partial(attend_half, static_h))

        def prod(n):
            d = ORDER[n]
            s = 6 + n // 2
            if n % 2 == 0:
                @pl.when(h == 0)
                def _():
                    wait_w(s)

            with scope("mm_out"):
                pb[h, d] = jnp.dot(o_buf[...], w[s, pl.ds((n % 2) * hw, hw), :],
                                   preferred_element_type=F32).astype(BF16)
            send(h, PAIR + d)
            if n % 2 == 1:
                @pl.when(h == 1)
                def _():
                    load(l, "d", 2 + n // 2, s)

        return [ln, qkv_main, qkv_rest, attend] + [functools.partial(prod, n) for n in range(4)]

    def mlp_steps(l, h):
        def ln():
            normalise(l, h, 1)

        def up(n):
            base = 8 + n * (4 * h - 8)

            @pl.when((h == 0) | (n == 1))
            def _():
                wait_w(*[base + r for r in range(4)])

            with scope("mm_up"):
                part = dot_all([a_buf[r] for r in range(4)], [w[base + r] for r in range(4)])
                h_buf[n] = jax.nn.gelu(part, approximate=True).astype(BF16)

            @pl.when(h == 1 - n)
            def _():
                for r in range(4):
                    load(l, "d", 4 + r, base + r)

            @pl.when(h * n == 1)
            def _():
                load_next(l, "q", 4, 4)
                load_next(l, "q", 5, 5)
                load_next(l, "o", 0, 6)
                load_next(l, "o", 1, 7)

        def prod(n):
            d = 2 + n + (n // 2) * (1 - 2 * n)
            s0 = lax.rem(4 + 2 * n, 8)
            s1 = 2 * n + 4 * (n // 2)
            s = s0 + h * (s1 - s0)
            wait_w(s, s + 1)
            with scope("mm_down"):
                part = dot_all([h_buf[0], h_buf[1]], [w[s], w[s + 1]])
                pb[h, d] = part.astype(BF16)
            send_pair(h, d)
            for k in range(4):
                for i in range(2):
                    @pl.when((n == k) & (h == 0))
                    def _():
                        if k < 2:
                            load(l, "u", 4 + 2 * k + i, s0 + i)
                        else:
                            load(l, "d", 2 * (k - 2) + i, s0 + i)

                    @pl.when((n == k) & (h == 1))
                    def _():
                        if k < 2:
                            if k == 1:
                                load_next(l, "q", 2 + i, Q_SLOTS[2 + i])
                        else:
                            load_next(l, "u", 2 * (k - 2) + i, s1 + i)

        return ln, up, prod

    def run_attn(l, h, plan):
        for n, step in enumerate(attn_steps(l, h)):
            step()
            for whose, ev in plan.get(n, ()):
                if whose == SELF:
                    ev(h)
                else:
                    pl.when(l + h > 0)(functools.partial(ev, 1 - h))

    def run_mlp(l, h, plan):
        ln, up, prod = mlp_steps(l, h)

        def events(n, k, at):
            for whose, ev in plan.get(at, ()):
                pl.when(n == k)(functools.partial(ev, h if whose == SELF else 1 - h))

        def up_step(n, c):
            up(n)
            for k in range(2):
                events(n, k, 1 + k)
            return c

        def prod_step(n, c):
            prod(n)
            for k in range(3):
                events(n, k, 3 + k)
            return c

        ln()
        lax.fori_loop(0, 2, up_step, 0)
        lax.fori_loop(0, num_chips, prod_step, 0)
        for whose, ev in plan[6]:
            ev(h if whose == SELF else 1 - h)

    def put_out(h):
        with scope("put"):
            for r in range(num_chips):
                out[pl.ds(h * rows, rows), block(r)] = xg[h, r]

    for r in range(num_chips):
        x_copy(0, r).start()
    load(0, "q", 0, Q_SLOTS[0])
    load(0, "q", 1, Q_SLOTS[1])
    barrier = pltpu.get_barrier_semaphore()
    for n in range(1, tp):
        pl.semaphore_signal(barrier, inc=1, device_id={"tp": lax.rem(me + n, tp)},
                            device_id_type=pl.DeviceIdType.MESH)
    qkv[...] = jnp.zeros_like(qkv)
    for k, gain in enumerate((g1, g2)):
        for l in range(num_layers):
            for r in range(num_chips):
                gains[k, l, r] = gain[pl.ds(l, 1), block(r)]
    for r in range(num_chips):
        x_copy(1, r).start()
    for r in range(2, 4):
        load(0, "q", r, Q_SLOTS[r])
    with scope("bar"):
        pl.semaphore_wait(barrier, tp - 1)

    def layer(l, c):
        def attn_half(h, c):
            run_attn(l, h, {
                1: [(OTHER, ev4)],
                5: [(OTHER, ev5)],
                6: [(SELF, ev1), (OTHER, ev6)],
                7: [(SELF, ev2_left), (SELF, ev2_right), (OTHER, ev_near_stats), (OTHER, ev7), (SELF, ev3), (OTHER, ev8)],
            })
            return c

        def mlp_half(h, c):
            run_mlp(l, h, {
                1: [(OTHER, ev4)],
                3: [(OTHER, ev5)],
                4: [(SELF, ev1)],
                5: [(OTHER, ev6), (SELF, ev2_left)],
                6: [(SELF, ev2_right), (OTHER, ev_near_stats), (OTHER, ev7), (SELF, ev3), (OTHER, ev8)],
            })
            return c

        lax.fori_loop(0, 2, attn_half, 0)
        lax.fori_loop(0, 2, mlp_half, 0)
        return c

    lax.fori_loop(0, num_layers, layer, 0)
    ev4(1)
    put_out(0)
    for ev in (ev5, ev6, ev_near, ev7, ev8):
        ev(1)
    put_out(1)


def solution(mesh):
    tp = mesh.shape["tp"]
    num_chips = tp // 2

    def device_fn(act_in, w_qkv, w_out, w_up, w_down, gain_one, gain_two):
        seq, model_dim = act_in.shape
        num_layers, _, heads, _, head_dim = w_qkv.shape
        ffn = w_up.shape[2]
        bw = model_dim // num_chips
        half, hw = seq // 2, bw // 2
        wq = jnp.transpose(w_qkv, (0, 2, 3, 1, 4)).reshape(num_layers, heads * 3, model_dim, head_dim)
        wo = w_out.reshape(num_layers, heads * head_dim, model_dim)
        vmem = pl.BlockSpec(memory_space=pltpu.VMEM)
        hbm = pl.BlockSpec(memory_space=pl.ANY)
        return pl.pallas_call(
            functools.partial(layer_kernel, num_layers, num_chips, heads, head_dim),
            out_shape=pltpu.VMEM((seq, model_dim), BF16),
            in_specs=[hbm] * 5 + [vmem] * 2,
            out_specs=vmem,
            scratch_shapes=[
                pltpu.VMEM((2, num_chips, half, bw), BF16),
                pltpu.VMEM((num_chips, half, bw), BF16),
                pltpu.VMEM((2, num_chips, half, bw), BF16),
                pltpu.VMEM((2, num_chips, half // 2, bw), BF16),
                pltpu.VMEM((2, 6, half // 2, hw), BF16),
                pltpu.VMEM((2, 6, half // 2, hw), BF16),
                pltpu.VMEM((heads * 3, seq, head_dim), BF16),
                pltpu.VMEM((half, heads * head_dim), BF16),
                pltpu.VMEM((ffn // bw, half, bw), BF16),
                pltpu.VMEM((2, num_layers, num_chips, 1, bw), F32),
                pltpu.VMEM((num_chips, 2, half, 128), F32),
                pltpu.VMEM((SLOTS, bw, bw), BF16),
                pltpu.SemaphoreType.DMA((SLOTS,)),
                pltpu.SemaphoreType.DMA((2, num_chips)),
                pltpu.SemaphoreType.DMA((2, KINDS, 2)),
                pltpu.SemaphoreType.DMA((2, KINDS, 2)),
            ],
            compiler_params=pltpu.CompilerParams(
                collective_id=0, has_side_effects=True, vmem_limit_bytes=60 * 2 ** 20),
            name="layers",
        )(act_in, wq, wo, w_up, w_down, gain_one, gain_two)

    return jax.shard_map(
        device_fn,
        mesh=mesh,
        in_specs=(
            P("dp", None),
            P(None, None, "tp", None, None),
            P(None, "tp", None, None),
            P(None, None, "tp"),
            P(None, "tp", None),
            P(None, None),
            P(None, None),
        ),
        out_specs=P("dp", None),
        check_vma=False,
    )
```

```python
import functools
import math

import jax
import jax.numpy as jnp
from jax import lax
from jax.experimental import pallas as pl
from jax.experimental.pallas import tpu as pltpu
from jax.sharding import PartitionSpec as P

F32 = jnp.float32
BF16 = jnp.bfloat16
SLOTS = 14
Q_SLOTS = (12, 13, 2, 3)
PAIR, M1R, M1L, M2R, M2L, M3R, M3L = 0, 4, 5, 6, 7, 8, 9
OWN_RA, OWN_RB, OWN_LA, OWN_LB, FWD_R, FWD_L = 10, 11, 12, 13, 14, 15
SH_OWN, SH_LA, SH_LB, SH_RA, SH_RB, SH_OA, SH_OB = 16, 17, 18, 19, 20, 21, 22
KINDS = 23
ORDER = (2, 3, 1, 0)
SPLIT = (M1R, M1L, M3R, M3L, OWN_RA, OWN_LB, FWD_R, FWD_L, SH_OA, SH_OB)
SELF, OTHER = 0, 1


def layer_kernel(
    num_layers, num_chips, heads, head_dim,
    x_hbm, wq, wo, w1, w2, g1, g2, out,
    xg, a_buf, pb, pr, sb, rb, qkv, o_buf, h_buf, gains, st, w,
    wsem, xsem, ssem, rsem,
):
    rows = xg.shape[2]
    bw = xg.shape[3]
    own = rows // 2
    hw = bw // 2
    model_dim = num_chips * bw
    tp = 2 * num_chips
    me = lax.axis_index("tp")
    chip = me // 2
    core = me % 2
    mine = pl.ds(pl.multiple_of(core * own, own), own)
    theirs = pl.ds(pl.multiple_of((1 - core) * own, own), own)
    scope = jax.named_scope

    def chip_at(r):
        return lax.rem(chip + r, num_chips)

    def block(r):
        return pl.ds(pl.multiple_of(chip_at(r) * bw, bw), bw)

    right = chip_at(1) * 2 + core
    left = chip_at(3) * 2 + core
    partner = chip * 2 + (1 - core)
    half_a = pl.ds(0, hw)
    half_b = pl.ds(hw, hw)

    def load(l, what, n, s):
        res = []

        def slab(t, r, col):
            res.append((wq.at[l, t, block(r), :], w.at[s, :, pl.ds(col, head_dim)]))

        if what == "q" and n < 4:
            for t in range(10):
                slab(t, n, t * head_dim)
        elif what == "q":
            for i in range(2):
                for t in range(5):
                    slab(10 + t, 2 * (n - 4) + i, i * hw + t * head_dim)
        elif what == "o":
            for i in range(2):
                res.append((wo.at[l, :, block(ORDER[2 * n + i])], w.at[s, pl.ds(i * hw, hw), :]))
        elif what == "u":
            res.append((w1.at[l, block(n % 4), pl.ds((n // 4) * bw, bw)], w.at[s]))
        else:
            res.append((w2.at[l, pl.ds((n % 2) * bw, bw), block(ORDER[n // 2])], w.at[s]))
        for a, b in res:
            pltpu.make_async_copy(a, b, wsem.at[s]).start()

    def load_next(l, what, n, s):
        @pl.when(l + 1 < num_layers)
        def _():
            load(l + 1, what, n, s)

    def wait_w(*slots):
        with scope("wwait"):
            for s in slots:
                pltpu.make_async_copy(w.at[s], w.at[s], wsem.at[s]).wait()

    part = own // 2

    def piece(p):
        return pl.ds(0, own) if p is None else pl.ds(p * part, part)

    def mine_of(p):
        return mine if p is None else pl.ds(pl.multiple_of(core * own + p * part, part), part)

    def msg(h, kind, p=None):
        n = 0 if p is None else p

        def rc(src, dst, dev):
            return pltpu.make_async_remote_copy(
                src_ref=src, dst_ref=dst, send_sem=ssem.at[h, kind, n], recv_sem=rsem.at[h, kind, n],
                device_id={"tp": dev}, device_id_type=pl.DeviceIdType.MESH,
            )

        def move(r_from, r_to, cols, dev):
            return rc(xg.at[h, r_from, mine_of(p), cols], xg.at[h, r_to, mine_of(p), cols], dev)

        if kind < 4:
            return rc(pb.at[h, kind, theirs, :], pr.at[h, kind], partner)
        if kind <= M3L:
            k = kind - M1R
            return rc(sb.at[h, k, piece(p), :], rb.at[h, k, piece(p), :], right if k % 2 == 0 else left)
        return move(*{
            OWN_RA: (0, 3, half_a, right), OWN_RB: (0, 3, half_b, right),
            OWN_LA: (0, 1, half_a, left), OWN_LB: (0, 1, half_b, left),
            FWD_R: (3, 2, half_a, right), FWD_L: (1, 2, half_b, left),
            SH_OWN: (0, 0, pl.ds(0, bw), partner),
            SH_LA: (3, 3, half_a, partner), SH_LB: (3, 3, half_b, partner),
            SH_RA: (1, 1, half_a, partner), SH_RB: (1, 1, half_b, partner),
            SH_OA: (2, 2, half_a, partner), SH_OB: (2, 2, half_b, partner),
        }[kind])

    def send_pair(h, d):
        pltpu.make_async_remote_copy(
            src_ref=pb.at[h, d, theirs, :], dst_ref=pr.at[h, d], send_sem=ssem.at[h, d, 0], recv_sem=rsem.at[h, d, 0],
            device_id={"tp": partner}, device_id_type=pl.DeviceIdType.MESH,
        ).start()

    def send(h, *kinds, p=None):
        for kind in kinds:
            msg(h, kind, p).start()

    def recv(h, *kinds, p=None):
        for kind in kinds:
            with scope("recv%d" % kind):
                msg(h, kind, p).wait_recv()

    def pair_sum(h, d, cols, p=None):
        return pb[h, d, mine_of(p), cols].astype(F32) + pr[h, d, piece(p), cols].astype(F32)

    def ev1(h):
        recv(h, PAIR + 2)
        for p in range(2):
            sb[h, 0, piece(p), :] = pair_sum(h, 2, half_a, p).astype(BF16)
            sb[h, 1, piece(p), :] = pair_sum(h, 2, half_b, p).astype(BF16)
            send(h, M1R, M1L, p=p)

    def ev2_left(h):
        recv(h, PAIR + 3)
        sb[h, 3] = pair_sum(h, 3, half_a).astype(BF16)
        send(h, M2L)

    def ev2_right(h):
        recv(h, PAIR + 1)
        sb[h, 2] = pair_sum(h, 1, half_b).astype(BF16)
        send(h, M2R)

    def ev3(h):
        for p in range(2):
            recv(h, M1R, p=p)
            sb[h, 4, piece(p), :] = (pair_sum(h, 1, half_a, p) + rb[h, 0, piece(p), :].astype(F32)).astype(BF16)
            send(h, M3R, p=p)
            recv(h, M1L, p=p)
            sb[h, 5, piece(p), :] = (pair_sum(h, 3, half_b, p) + rb[h, 1, piece(p), :].astype(F32)).astype(BF16)
            send(h, M3L, p=p)

    def ev4(h):
        recv(h, PAIR + 0, M2L, M2R)

        def own_sum(cols, plain, summed, p):
            xg[h, 0, mine_of(p), cols] = (xg[h, 0, mine_of(p), cols].astype(F32) + (
                pair_sum(h, 0, cols, p) + rb[h, plain, piece(p), :].astype(F32)
                + rb[h, summed, piece(p), :].astype(F32))).astype(BF16)

        for p in range(2):
            recv(h, M3R, p=p)
            own_sum(half_a, 3, 4, p)
            send(h, OWN_RA, p=p)
            recv(h, M3L, p=p)
            own_sum(half_b, 2, 5, p)
            send(h, OWN_LB, p=p)
        send(h, OWN_LA, OWN_RB, SH_OWN)

    def ev5(h):
        for p in range(2):
            recv(h, OWN_RA, p=p)
            send(h, FWD_R, p=p)
            recv(h, OWN_LB, p=p)
            send(h, FWD_L, p=p)
        send(h, SH_LA, SH_RB)

    def ev6(h):
        recv(h, OWN_LA)
        send(h, SH_RA)
        recv(h, OWN_RB)
        send(h, SH_LB)

    def ev7(h):
        for p in range(2):
            recv(h, FWD_R, p=p)
            send(h, SH_OA, p=p)
            recv(h, FWD_L, p=p)
            send(h, SH_OB, p=p)

    def ev_near(h):
        recv(h, SH_OWN, SH_LA, SH_LB, SH_RA, SH_RB)

    def ev_near_stats(h):
        ev_near(h)
        near_stats(h)

    def ev8(h):
        for p in range(2):
            recv(h, SH_OA, SH_OB, p=p)
        with scope("sent"):
            for kind in range(KINDS):
                for p in (0, 1) if kind in SPLIT else (None,):
                    msg(h, kind, p).wait_send()

    def x_copy(h, r):
        src = x_hbm.at[pl.ds(pl.multiple_of(h * rows, rows), rows), block(r)]
        return pltpu.make_async_copy(src, xg.at[h, r], xsem.at[h, r])

    tiles = bw // 128

    def x_tile(h, r, t):
        return xg[h, r, :, t * 128:(t + 1) * 128].astype(F32)

    def block_stats(h, r):
        total = x_tile(h, r, 0)
        for t in range(1, tiles):
            total = total + x_tile(h, r, t)
        mean = jnp.sum(total, axis=1, keepdims=True) * (1.0 / bw)
        sq = jnp.zeros((rows, 128), F32)
        for t in range(tiles):
            d = x_tile(h, r, t) - mean
            sq = sq + d * d
        m2 = jnp.sum(sq, axis=1, keepdims=True)
        st[r, 0] = jnp.broadcast_to(mean, (rows, 128))
        st[r, 1] = jnp.broadcast_to(m2, (rows, 128))

    def near_stats(h):
        def one(n, c):
            block_stats(h, n + n // 2)
            return c

        with scope("stats"):
            lax.fori_loop(0, num_chips - 1, one, 0)

    def normalise(l, h, which):
        with scope("norm"):
            block_stats(h, 2)
            mean = (st[0, 0] + st[1, 0] + st[2, 0] + st[3, 0]) * (1.0 / num_chips)
            m2 = st[0, 1] + st[1, 1] + st[2, 1] + st[3, 1]
            for r in range(num_chips):
                d = st[r, 0] - mean
                m2 = m2 + bw * (d * d)
            rstd = lax.rsqrt(m2 * (1.0 / model_dim) + 1e-5)

            def scaled(r, c):
                for t in range(tiles):
                    g = gains[which, l, r, :, t * 128:(t + 1) * 128]
                    a_buf[r, :, t * 128:(t + 1) * 128] = ((x_tile(h, r, t) - mean) * rstd * g).astype(BF16)
                return c

            lax.fori_loop(0, num_chips, scaled, 0)

    def dot_all(lhs, rhs):
        return sum(jnp.dot(a, b, preferred_element_type=F32) for a, b in zip(lhs, rhs))

    def attn_steps(l, h):
        my_rows = pl.ds(pl.multiple_of(h * rows, rows), rows)

        def ln():
            @pl.when(l == 0)
            def _():
                for r in range(num_chips):
                    x_copy(h, r).wait()
                near_stats(h)

            normalise(l, h, 0)

            @pl.when(l + h == 0)
            def _():
                load(0, "q", 4, 4)
                load(0, "q", 5, 5)
                load(0, "o", 0, 6)
                load(0, "o", 1, 7)

        def qkv_main():
            @pl.when(h == 0)
            def _():
                wait_w(*Q_SLOTS)

            with scope("mm_qkv"):
                for first, count in ((0, 4), (4, 4), (8, 2)):
                    part = dot_all([a_buf[r] for r in range(4)],
                                   [w[s, :, pl.ds(first * head_dim, count * head_dim)] for s in Q_SLOTS])
                    for t in range(count):
                        qkv[first + t, my_rows, :] = part[:, t * head_dim:(t + 1) * head_dim].astype(BF16)

            @pl.when(h == 1)
            def _():
                for r in range(4):
                    load(l, "u", 4 + r, r)
                load_next(l, "q", 0, Q_SLOTS[0])
                load_next(l, "q", 1, Q_SLOTS[1])

            @pl.when(l + h == 0)
            def _():
                for r in range(4):
                    load(0, "u", r, 8 + r)

        def qkv_rest():
            @pl.when(h == 0)
            def _():
                wait_w(4, 5)

            with scope("mm_qkv2"):
                for first, count in ((0, 4), (4, 1)):
                    part = dot_all([a_buf[r] for r in range(4)],
                                   [w[4 + r // 2, :, pl.ds((r % 2) * hw + first * head_dim, count * head_dim)]
                                    for r in range(4)])
                    for t in range(count):
                        qkv[10 + first + t, my_rows, :] = part[:, t * head_dim:(t + 1) * head_dim].astype(BF16)

            @pl.when(h == 1)
            def _():
                load(l, "d", 0, 4)
                load(l, "d", 1, 5)

        def attend_half(static_h):
            at = pl.ds(static_h * rows, rows)
            shape = (rows, 2 * rows)
            q_pos = static_h * rows + lax.broadcasted_iota(jnp.int32, shape, 0)
            keep = lax.broadcasted_iota(jnp.int32, shape, 1) <= q_pos
            scale = 1.0 / math.sqrt(head_dim)
            with scope("attn"):
                for n in range(heads):
                    s = lax.dot_general(qkv[3 * n, at, :], qkv[3 * n + 1], (((1,), (1,)), ((), ())),
                                        preferred_element_type=F32) * scale
                    s = jnp.where(keep, s, -1e30)
                    p = jnp.exp(s - jnp.max(s, axis=1, keepdims=True))
                    total = jnp.sum(p, axis=1, keepdims=True)
                    mix = jnp.dot(p.astype(BF16), qkv[3 * n + 2], preferred_element_type=F32)
                    o_buf[:, n * head_dim:(n + 1) * head_dim] = (mix / total).astype(BF16)

        def attend():
            for static_h in range(2):
                pl.when(h == static_h)(functools.partial(attend_half, static_h))

        def prod(n):
            d = ORDER[n]
            s = 6 + n // 2
            if n % 2 == 0:
                @pl.when(h == 0)
                def _():
                    wait_w(s)

            with scope("mm_out"):
                pb[h, d] = jnp.dot(o_buf[...], w[s, pl.ds((n % 2) * hw, hw), :],
                                   preferred_element_type=F32).astype(BF16)
            send(h, PAIR + d)
            if n % 2 == 1:
                @pl.when(h == 1)
                def _():
                    load(l, "d", 2 + n // 2, s)

        return [ln, qkv_main, qkv_rest, attend] + [functools.partial(prod, n) for n in range(4)]

    def mlp_steps(l, h):
        def ln():
            normalise(l, h, 1)

        def up(n):
            base = 8 + n * (4 * h - 8)

            @pl.when((h == 0) | (n == 1))
            def _():
                wait_w(*[base + r for r in range(4)])

            with scope("mm_up"):
                part = dot_all([a_buf[r] for r in range(4)], [w[base + r] for r in range(4)])
                h_buf[n] = jax.nn.gelu(part, approximate=True).astype(BF16)

            @pl.when(h == 1 - n)
            def _():
                for r in range(4):
                    load(l, "d", 4 + r, base + r)

            @pl.when(h * n == 1)
            def _():
                load_next(l, "q", 4, 4)
                load_next(l, "q", 5, 5)
                load_next(l, "o", 0, 6)
                load_next(l, "o", 1, 7)

        def prod(n):
            d = 2 + n + (n // 2) * (1 - 2 * n)
            s0 = lax.rem(4 + 2 * n, 8)
            s1 = 2 * n + 4 * (n // 2)
            s = s0 + h * (s1 - s0)
            wait_w(s, s + 1)
            with scope("mm_down"):
                part = dot_all([h_buf[0], h_buf[1]], [w[s], w[s + 1]])
                pb[h, d] = part.astype(BF16)
            send_pair(h, d)
            for k in range(4):
                for i in range(2):
                    @pl.when((n == k) & (h == 0))
                    def _():
                        if k < 2:
                            load(l, "u", 4 + 2 * k + i, s0 + i)
                        else:
                            load(l, "d", 2 * (k - 2) + i, s0 + i)

                    @pl.when((n == k) & (h == 1))
                    def _():
                        if k < 2:
                            if k == 1:
                                load_next(l, "q", 2 + i, Q_SLOTS[2 + i])
                        else:
                            load_next(l, "u", 2 * (k - 2) + i, s1 + i)

        return ln, up, prod

    def run_attn(l, h, plan):
        for n, step in enumerate(attn_steps(l, h)):
            step()
            for whose, ev in plan.get(n, ()):
                if whose == SELF:
                    ev(h)
                else:
                    pl.when(l + h > 0)(functools.partial(ev, 1 - h))

    def run_mlp(l, h, plan):
        ln, up, prod = mlp_steps(l, h)

        def events(n, k, at):
            for whose, ev in plan.get(at, ()):
                pl.when(n == k)(functools.partial(ev, h if whose == SELF else 1 - h))

        def up_step(n, c):
            up(n)
            for k in range(2):
                events(n, k, 1 + k)
            return c

        def prod_step(n, c):
            prod(n)
            for k in range(3):
                events(n, k, 3 + k)
            return c

        ln()
        lax.fori_loop(0, 2, up_step, 0)
        lax.fori_loop(0, num_chips, prod_step, 0)
        for whose, ev in plan[6]:
            ev(h if whose == SELF else 1 - h)

    def put_out(h):
        with scope("put"):
            for r in range(num_chips):
                out[pl.ds(h * rows, rows), block(r)] = xg[h, r]

    for r in range(num_chips):
        x_copy(0, r).start()
    load(0, "q", 0, Q_SLOTS[0])
    load(0, "q", 1, Q_SLOTS[1])
    barrier = pltpu.get_barrier_semaphore()
    for n in range(1, tp):
        pl.semaphore_signal(barrier, inc=1, device_id={"tp": lax.rem(me + n, tp)},
                            device_id_type=pl.DeviceIdType.MESH)
    qkv[...] = jnp.zeros_like(qkv)
    for k, gain in enumerate((g1, g2)):
        for l in range(num_layers):
            for r in range(num_chips):
                gains[k, l, r] = gain[pl.ds(l, 1), block(r)]
    for r in range(num_chips):
        x_copy(1, r).start()
    for r in range(2, 4):
        load(0, "q", r, Q_SLOTS[r])
    with scope("bar"):
        pl.semaphore_wait(barrier, tp - 1)

    def layer(l, c):
        def attn_half(h, c):
            run_attn(l, h, {
                1: [(OTHER, ev4)],
                6: [(OTHER, ev5), (SELF, ev1), (OTHER, ev6)],
                7: [(SELF, ev2_left), (SELF, ev2_right), (OTHER, ev_near_stats), (OTHER, ev7), (SELF, ev3), (OTHER, ev8)],
            })
            return c

        def mlp_half(h, c):
            run_mlp(l, h, {
                1: [(OTHER, ev4)],
                4: [(OTHER, ev5), (SELF, ev1)],
                5: [(OTHER, ev6), (SELF, ev2_left)],
                6: [(SELF, ev2_right), (OTHER, ev_near_stats), (OTHER, ev7), (SELF, ev3), (OTHER, ev8)],
            })
            return c

        lax.fori_loop(0, 2, attn_half, 0)
        lax.fori_loop(0, 2, mlp_half, 0)
        return c

    lax.fori_loop(0, num_layers, layer, 0)
    ev4(1)
    put_out(0)
    for ev in (ev5, ev6, ev_near, ev7, ev8):
        ev(1)
    put_out(1)


def solution(mesh):
    tp = mesh.shape["tp"]
    num_chips = tp // 2

    def device_fn(act_in, w_qkv, w_out, w_up, w_down, gain_one, gain_two):
        seq, model_dim = act_in.shape
        num_layers, _, heads, _, head_dim = w_qkv.shape
        ffn = w_up.shape[2]
        bw = model_dim // num_chips
        half, hw = seq // 2, bw // 2
        wq = jnp.transpose(w_qkv, (0, 2, 3, 1, 4)).reshape(num_layers, heads * 3, model_dim, head_dim)
        wo = w_out.reshape(num_layers, heads * head_dim, model_dim)
        vmem = pl.BlockSpec(memory_space=pltpu.VMEM)
        hbm = pl.BlockSpec(memory_space=pl.ANY)
        return pl.pallas_call(
            functools.partial(layer_kernel, num_layers, num_chips, heads, head_dim),
            out_shape=pltpu.VMEM((seq, model_dim), BF16),
            in_specs=[hbm] * 5 + [vmem] * 2,
            out_specs=vmem,
            scratch_shapes=[
                pltpu.VMEM((2, num_chips, half, bw), BF16),
                pltpu.VMEM((num_chips, half, bw), BF16),
                pltpu.VMEM((2, num_chips, half, bw), BF16),
                pltpu.VMEM((2, num_chips, half // 2, bw), BF16),
                pltpu.VMEM((2, 6, half // 2, hw), BF16),
                pltpu.VMEM((2, 6, half // 2, hw), BF16),
                pltpu.VMEM((heads * 3, seq, head_dim), BF16),
                pltpu.VMEM((half, heads * head_dim), BF16),
                pltpu.VMEM((ffn // bw, half, bw), BF16),
                pltpu.VMEM((2, num_layers, num_chips, 1, bw), F32),
                pltpu.VMEM((num_chips, 2, half, 128), F32),
                pltpu.VMEM((SLOTS, bw, bw), BF16),
                pltpu.SemaphoreType.DMA((SLOTS,)),
                pltpu.SemaphoreType.DMA((2, num_chips)),
                pltpu.SemaphoreType.DMA((2, KINDS, 2)),
                pltpu.SemaphoreType.DMA((2, KINDS, 2)),
            ],
            compiler_params=pltpu.CompilerParams(
                collective_id=0, has_side_effects=True, vmem_limit_bytes=60 * 2 ** 20),
            name="layers",
        )(act_in, wq, wo, w_up, w_down, gain_one, gain_two)

    return jax.shard_map(
        device_fn,
        mesh=mesh,
        in_specs=(
            P("dp", None),
            P(None, None, "tp", None, None),
            P(None, "tp", None, None),
            P(None, None, "tp"),
            P(None, "tp", None),
            P(None, None),
            P(None, None),
        ),
        out_specs=P("dp", None),
        check_vma=False,
    )
```
